256 devices in a mesh: gx: 8 (over z_lo, core), gy: 32 (over z_hi, y, x).
Axes of the slice: x: 4, y: 4, z: 8 (z_hi: 2, z_lo: 4; z = z_hi * 4 + z_lo), core: 2. Of those that a mesh axis runs over, the one named last changes fastest.
Arguments:
- density: float32 [128, 512, 256], P('gx', 'gy'), may hold values from 0.5 to 2
- momentum: float32 [3, 128, 512, 256], P(None, 'gx', 'gy'), may hold values from -3 to 3
- energy: float32 [128, 512, 256], P('gx', 'gy'), may hold values from 1 to 3
- parcel_mass: float32 [2097152], P(('gx', 'gy')), may hold values from 0.2 to 2
- droplet_velocity: float32 [3, 2097152], P(None, ('gx', 'gy')), may hold values from -4 to 4
- parcel_temp: float32 [2097152], P(('gx', 'gy')), may hold values from 0.1 to 4
- parcel_cell: int32 [3, 2097152], P(None, ('gx', 'gy')), may hold values from 0 to 511, as said below
- parcel_count: int32 [256], P(('gx', 'gy')), may hold values from 2048 to 8192, as said below
Outputs:
- updated_fluid_density: float32 [128, 512, 256], P('gx', 'gy')
- updated_fluid_impulse: float32 [3, 128, 512, 256], P(None, 'gx', 'gy')
- energy_out: float32 [128, 512, 256], P('gx', 'gy')
- moved_state: float32 [5, 2621440], P(None, ('gx', 'gy'))
- moved_cell: int32 [3, 2621440], P(None, ('gx', 'gy'))
- time_step: float32 [], replicated
The draws below stay inside these ranges and needn't reach their ends.
Inputs may be any that keep to these rules, and one draw needn't show every extreme that they name: `parcel_cell`: each row of device d lies in d's block of 16 x 16 x 256 cells or in the layer of cells just beyond one of its four side faces inside the grid, never beyond an edge. Among the live rows of one device at most 512 lie beyond any one face; on every device some face along each of the two axes has exactly 512. `parcel_count`: some devices are full.
All inputs are finite; a program needn't handle non-finite values.
Results may differ from the reference program's by a relative error of at most 0.0003.
Values sent between devices are 32-bit elements; how exact they have to be, the bound alone decides.
A program may use at most 192 MiB of HBM per device.

```python
import math
import jax
import jax.numpy as jnp
from jax import lax

CX = 16
CY = 16
NZ = 256
P_DEV = 8192
MOVE = 512
SLOTS = 10240
NX = 128
NY = 512
PARCELS = 2097152
N_GX = 8
N_GY = 32
DEVICES = 256


def parcel_state_tables(key):
    base = jax.random.fold_in(key, 11)
    keys = jax.random.split(base, 8)
    device = jnp.arange(DEVICES, dtype=jnp.int32)
    col_x = device // N_GY
    col_y = device % N_GY
    partial_parcel_count = jax.random.randint(keys[0], (DEVICES,), P_DEV // 4, P_DEV // 2 + 1, dtype=jnp.int32)
    count = jnp.where(col_x == 0, P_DEV, partial_parcel_count).astype(jnp.int32)
    exists = jnp.stack([col_x > 0, col_x < N_GX - 1, col_y > 0, col_y < N_GY - 1], axis=1)
    loads = jax.random.randint(keys[1], (DEVICES, 4), MOVE // 4, MOVE + 1, dtype=jnp.int32)
    drag_horizontal = jnp.where(col_x < N_GX - 1, 1, 0)
    force_y = jnp.where(col_y < N_GY - 1, 3, 2)
    which = jnp.arange(4, dtype=jnp.int32)[None]
    loads = jnp.where((which == drag_horizontal[:, None]) | (which == force_y[:, None]), MOVE, loads)
    loads = jnp.where(exists, loads, 0)
    ends = jnp.cumsum(loads, axis=1)
    row_index = jnp.arange(P_DEV, dtype=jnp.int32)[None]
    spread = 2 ** 30 // (2 * P_DEV)
    scores = jax.random.randint(keys[2], (DEVICES, P_DEV), 0, spread, dtype=jnp.int32) * P_DEV + row_index
    scores = jnp.where(row_index < count[:, None], scores, 2 ** 30 + row_index)
    order = jnp.argsort(scores, axis=1, stable=True)
    position = jnp.argsort(order, axis=1, stable=True).astype(jnp.int32)
    heading = jnp.sum((position[:, :, None] >= ends[:, None, :]).astype(jnp.int32), axis=2)
    inside_x = jax.random.randint(keys[3], (DEVICES, P_DEV), 0, CX, dtype=jnp.int32) + col_x[:, None] * CX
    inside_y = jax.random.randint(keys[4], (DEVICES, P_DEV), 0, CY, dtype=jnp.int32) + col_y[:, None] * CY
    depth = jax.random.randint(keys[5], (DEVICES, P_DEV), 0, NZ, dtype=jnp.int32)
    cell_x = jnp.where(heading == 0, col_x[:, None] * CX - 1, jnp.where(heading == 1, col_x[:, None] * CX + CX, inside_x))
    cell_y = jnp.where(heading == 2, col_y[:, None] * CY - 1, jnp.where(heading == 3, col_y[:, None] * CY + CY, inside_y))
    cells = jnp.stack([cell_x, cell_y, depth]).reshape(3, DEVICES * P_DEV).astype(jnp.int32)
    return (cells, count)


def draw_parcel_cell(key, part):
    return parcel_state_tables(key)[0]


def draw_parcel_count(key, part):
    return parcel_state_tables(key)[1]


def level_of(stream_key, dims, cuts, smallest, top_value):
    loudness = 1.0
    for dim, blocks in cuts:
        heights = jax.random.uniform(jax.random.fold_in(jax.random.fold_in(stream_key, 6), dim), (blocks,), jnp.float32, smallest / len(cuts), top_value / len(cuts))
        loudness = loudness * jnp.repeat(jnp.exp(heights), dims[dim] // blocks).reshape((-1,) + (1,) * (len(dims) - 1 - dim))
    return loudness


def noise(stream_key, extent, deviation, reach, shards=(), held_as=jnp.bfloat16):
    values = jax.random.normal(stream_key, extent, jnp.float32) * deviation
    if len(shards) > 0:
        values = level_of(stream_key, extent, shards, -0.22, 0.18) * values
    return jnp.clip(values, min=-reach, max=reach).astype(held_as)


def setup_inputs(seed: int = 0) -> dict:
    key_of = jax.random.split(jax.random.key(seed), 9)
    density = jnp.clip(0.5 + 1.5 * jax.random.uniform(key_of[0], (NX, NY, NZ), jnp.float32) ** level_of(key_of[0], (NX, NY, NZ), ((0, 8), (1, 32)), -0.2, 0.2), 0.5, 2.0)
    momentum = noise(key_of[1], (3, NX, NY, NZ), 0.5, 3.0, ((1, 8), (2, 32)), jnp.float32)
    energy = jnp.clip(1.0 + 2.0 * jax.random.uniform(key_of[2], (NX, NY, NZ), jnp.float32) ** level_of(key_of[2], (NX, NY, NZ), ((0, 8), (1, 32)), -0.2, 0.2), 1.0, 3.0)
    parcel_mass = jnp.clip(jnp.exp(math.log(2.0) - 2.3025851 * jax.random.uniform(key_of[3], (PARCELS,), jnp.float32) ** level_of(key_of[3], (PARCELS,), ((0, 256),), -0.2, 0.2)), 0.2, 2.0)
    droplet_velocity = noise(key_of[4], (3, PARCELS), 1.0, 4.0, ((1, 256),), jnp.float32)
    parcel_temp = jnp.clip(0.1 + 3.9 * jax.random.uniform(key_of[5], (PARCELS,), jnp.float32) ** level_of(key_of[5], (PARCELS,), ((0, 256),), -0.2, 0.2), 0.1, 4.0)
    parcel_cell = draw_parcel_cell(jax.random.fold_in(key_of[8], 71), 0)
    parcel_count = draw_parcel_count(jax.random.fold_in(key_of[8], 71), 0)
    return dict(density=density, momentum=momentum, energy=energy, parcel_mass=parcel_mass, droplet_velocity=droplet_velocity, parcel_temp=parcel_temp, parcel_cell=parcel_cell, parcel_count=parcel_count)


ADIABATIC_INDEX = 1.4
KICK = 0.25
COURANT = 0.4
SHRINK = 0.5

def cell_sums(values, cell_ids, segments):
    return jax.ops.segment_sum(values, cell_ids, num_segments=segments)

def reference(density, momentum, energy, parcel_mass, droplet_velocity, parcel_temp, parcel_cell, parcel_count):
    row_index = jnp.arange(parcel_mass.shape[0], dtype=jnp.int32)
    device = row_index // P_DEV
    local_row = row_index % P_DEV
    live = local_row < parcel_count[device]
    boiled_off_amount = jnp.where(live, parcel_mass * jax.nn.sigmoid(2.0 * (parcel_temp - 2.0)), 0.0)
    specific_movement_budget = 0.5 * lax.optimization_barrier(jnp.sum(droplet_velocity * droplet_velocity, axis=0))
    sources = jnp.concatenate([boiled_off_amount[None], boiled_off_amount[None] * droplet_velocity, (boiled_off_amount * (parcel_temp + specific_movement_budget))[None]], axis=0)
    flat_cell = (parcel_cell[0] * NY + parcel_cell[1]) * NZ + parcel_cell[2]
    deposit = jax.vmap(lambda values: cell_sums(values, flat_cell, NX * NY * NZ))(sources).reshape(5, NX, NY, NZ)
    updated_fluid_density = density + deposit[0]
    energy_out = energy + deposit[4]
    lifted = momentum + deposit[1:4]
    normal_stress_field = (ADIABATIC_INDEX - 1.0) * energy_out
    padded = jnp.pad(normal_stress_field, 1)
    grad_x = 0.5 * (padded[2:, 1:-1, 1:-1] - padded[:-2, 1:-1, 1:-1])
    grad_y = 0.5 * (padded[1:-1, 2:, 1:-1] - padded[1:-1, :-2, 1:-1])
    grad_z = 0.5 * (padded[1:-1, 1:-1, 2:] - padded[1:-1, 1:-1, :-2])
    updated_fluid_impulse = lifted - KICK * jnp.stack([grad_x, grad_y, grad_z])
    ambient_stream_speed = updated_fluid_impulse / updated_fluid_density[None]
    acoustic_signal = lax.optimization_barrier(jnp.max(jnp.abs(ambient_stream_speed), axis=0)) + jnp.sqrt(ADIABATIC_INDEX * normal_stress_field / updated_fluid_density)
    time_step = COURANT / jnp.max(acoustic_signal)
    col_x = device // N_GY
    col_y = device % N_GY
    local_x = parcel_cell[0] - col_x * CX
    local_y = parcel_cell[1] - col_y * CY
    heading = jnp.where(local_x < 0, 0, jnp.where(local_x >= CX, 1, jnp.where(local_y < 0, 2, jnp.where(local_y >= CY, 3, 4))))
    heading = jnp.where(live, heading, 5).astype(jnp.int32)
    onehot = (heading[:, None] == jnp.arange(4, dtype=jnp.int32)[None]).astype(jnp.int32).reshape(DEVICES, P_DEV, 4)
    earlier = (jnp.cumsum(onehot, axis=1) - onehot).reshape(DEVICES * P_DEV, 4)
    rank = lax.optimization_barrier(jnp.sum(earlier * onehot.reshape(DEVICES * P_DEV, 4), axis=1))
    shift_table = jnp.array([-N_GY, N_GY, -1, 1, 0, 0], dtype=jnp.int32)
    bucket_table = jnp.array([1, 0, 3, 2, 0, 0], dtype=jnp.int32)
    target_dev = device + shift_table[heading]
    moving = jnp.where(heading < 4, target_dev * SLOTS + P_DEV + bucket_table[heading] * MOVE + rank, SLOTS * DEVICES)
    target = jnp.where(heading == 4, device * SLOTS + local_row, moving).astype(jnp.int32)
    carried_records = jnp.concatenate([(parcel_mass - SHRINK * boiled_off_amount)[None], droplet_velocity, parcel_temp[None], parcel_cell.astype(jnp.float32)], axis=0)
    table = jnp.zeros((8, SLOTS * DEVICES), carried_records.dtype).at[:, target].set(carried_records, mode='drop')
    moved_state = table[:5]
    moved_cell = table[5:].astype(jnp.int32)
    return (updated_fluid_density, updated_fluid_impulse, energy_out, moved_state, moved_cell, time_step)
```

```python
import functools

import jax
import jax.numpy as jnp
from jax import lax
from jax.experimental import pallas as pl
from jax.experimental.pallas import tpu as pltpu
from jax.sharding import PartitionSpec as P

ADIABATIC_INDEX = 1.4
KICK = 0.25
COURANT = 0.4
SHRINK = 0.5
FACES = 4
F32 = jnp.float32
BF16 = jnp.bfloat16
MESH = pl.DeviceIdType.MESH
VMEM = pltpu.VMEM
ANY = pl.ANY


def row_iota(shape):
    return lax.broadcasted_iota(jnp.int32, shape, 0)


def lane_iota(shape):
    return lax.broadcasted_iota(jnp.int32, shape, 1)


def pack_left(cells, shift, steps):
    width = cells.shape[1]
    for k in range(steps):
        step = 1 << k
        coming = pltpu.roll(cells, width - step, axis=1)
        coming_shift = pltpu.roll(shift, width - step, axis=1)
        take = (coming_shift & step) != 0
        leave = (shift & step) != 0
        cells = jnp.where(take, coming, cells)
        shift = jnp.where(take, coming_shift, jnp.where(leave, 0, shift))
    return cells, shift


def sort_kernel(cells_x, cells_y, mass, vel, temp, cell, count, stay_out, bucket_out):
    rows = mass.shape[1]
    move = rows // 16
    chunk = 256
    chunks = rows // chunk
    anchor_x = lax.axis_index("gx") * cells_x
    anchor_y = lax.axis_index("gy") * cells_y
    live = lane_iota((1, rows)) < count[0]
    m, t = mass[...], temp[...]
    boiled = m * (1.0 / (1.0 + jnp.exp(4.0 - 2.0 * t)))
    left = m - SHRINK * boiled
    local_x = cell[0:1, :] - anchor_x
    local_y = cell[1:2, :] - anchor_y
    heading = jnp.where(
        local_x < 0,
        0,
        jnp.where(
            local_x >= cells_x, 1, jnp.where(local_y < 0, 2, jnp.where(local_y >= cells_y, 3, 4))
        ),
    )
    heading = jnp.where(live, heading, 5)
    record = jnp.concatenate([left, vel[...], t, cell[...].astype(F32)], axis=0)
    heads = jnp.broadcast_to(heading, (8, rows))
    stay_out[...] = jnp.where(heads == 4, record, 0.0)

    sub = row_iota((8, rows))
    mask = jnp.where((sub == heads) & (sub < 4), 1.0, 0.0)
    mask = jnp.where((sub == 4) & (heads < 4), 1.0, mask)
    stacked = jnp.concatenate(
        [mask[:, c * chunk : (c + 1) * chunk] for c in range(chunks)], axis=0
    ).astype(BF16)
    a, b = row_iota((chunk, chunk)), lane_iota((chunk, chunk))
    upper = jnp.where(a < b, 1.0, 0.0).astype(BF16)
    inside = jnp.dot(stacked, upper, preferred_element_type=F32)
    total = jnp.dot(stacked, jnp.ones((chunk, chunk), BF16), preferred_element_type=F32)
    n = 8 * chunks
    a, b = row_iota((n, n)), lane_iota((n, n))
    ahead = jnp.where(((a & 7) == (b & 7)) & (b < a), 1.0, 0.0).astype(BF16)
    before = jnp.dot(ahead, total.astype(BF16), preferred_element_type=F32)
    ranks = inside + before
    rank = jnp.concatenate([ranks[c * 8 : (c + 1) * 8] for c in range(chunks)], axis=1)
    counts = (before + total)[n - 8 : n, :128].astype(jnp.int32)

    own = jnp.sum(jnp.where(sub < 4, mask * rank, 0.0), axis=0, keepdims=True).astype(jnp.int32)
    overall = rank[4:5].astype(jnp.int32)
    moves = heading < 4
    shift = lane_iota((1, rows)) - overall
    target = heading * move + own
    shift = jnp.where(moves, shift + target * rows, 0)
    packed, key = pack_left(record, jnp.broadcast_to(shift, (8, rows)), rows.bit_length() - 1)

    wide = FACES * move
    packed = packed[:, :wide]
    slot = key[:, :wide] // rows
    place = lane_iota((8, wide))
    present = place < jnp.concatenate([counts[4:5]] * (wide // 128), axis=1)
    for h in range(FACES):
        mine = present & (slot // move == h)
        gap = jnp.where(mine, place - (slot - h * move), 0)
        out, _ = pack_left(packed, gap, wide.bit_length() - 1)
        full = jnp.concatenate([counts[h : h + 1]] * (move // 128), axis=1)
        bucket_out[h] = jnp.where(lane_iota((8, move)) < full, out[:, :move], 0.0)


def main_kernel(
    nx,
    ny,
    cells_x,
    cells_y,
    stay,
    bucket,
    density,
    momentum,
    energy,
    density_out,
    momentum_out,
    energy_out,
    arrived_out,
    step_out,
    dens,
    mom,
    ener,
    press,
    dep,
    got,
    side,
    halo,
    best,
    best_in,
    load_sem,
    store_sem,
    bucket_send,
    bucket_recv,
    halo_send,
    halo_recv,
    best_send,
    best_recv,
):
    i, j = lax.axis_index("gx"), lax.axis_index("gy")
    cols = cells_x * cells_y
    depth = press.shape[1]
    rows = stay.shape[1]
    move = got.shape[2]
    up_x, down_x = lax.rem(i + 1, nx), lax.rem(i + nx - 1, nx)
    up_y, down_y = lax.rem(j + 1, ny), lax.rem(j + ny - 1, ny)
    near = [(down_x, j), (up_x, j), (i, down_y), (i, up_y)]
    half = ny // 2
    spot = lax.div(j, half) * nx + i
    lane = lax.rem(j, half)
    size_a, size_b = 2 * nx, half
    first = []
    for q in range(1, size_a):
        there = lax.rem(spot + q, size_a)
        first.append((lax.rem(there, nx), lax.div(there, nx) * half + lane))
    second = []
    for q in range(1, size_b):
        second.append((i, lax.div(j, half) * half + lax.rem(lane + q, size_b)))

    barrier = pltpu.get_barrier_semaphore()
    everyone = near + first + second
    for peer in everyone:
        pl.semaphore_signal(barrier, inc=1, device_id=peer, device_id_type=MESH)

    loads = [
        pltpu.make_async_copy(energy, ener, load_sem.at[0]),
        pltpu.make_async_copy(density, dens, load_sem.at[1]),
        pltpu.make_async_copy(momentum, mom, load_sem.at[2]),
    ]
    for load in loads:
        load.start()

    anchor_x, anchor_y = i * cells_x, j * cells_y

    def terms(table, fields):
        v = table[1:4]
        t = table[4:5]
        boiled = table[0:1] / (0.5 + jnp.exp(4.0 - 2.0 * t))
        parts = []
        for f in fields:
            if f == 0:
                s = boiled
            elif f < 4:
                s = boiled * v[f - 1 : f]
            else:
                s = boiled * (t + 0.5 * jnp.sum(v * v, axis=0, keepdims=True))
            high = s.astype(BF16)
            low = (s - high.astype(F32)).astype(BF16)
            parts.append((high, low))
        width = table.shape[1]
        local = table[5:6].astype(jnp.int32) - anchor_x
        local = local * cells_y + table[6:7].astype(jnp.int32) - anchor_y
        column = jnp.where((local >= 0) & (local < cols), local, -1).astype(F32).astype(BF16)
        deep = table[7:8].astype(BF16)
        return parts, column, deep

    def deposit(table, fields):
        parts, column, deep = terms(table, fields)
        width = table.shape[1]
        which = row_iota((cols, width)).astype(F32).astype(BF16)
        there = which == column
        layer = row_iota((depth, width)).astype(F32).astype(BF16)
        pick = jnp.where(layer == deep, BF16(1), BF16(0))
        for f, halves in zip(fields, parts):
            both = jnp.concatenate([jnp.where(there, s, BF16(0)) for s in halves], axis=0)
            sums = lax.dot_general(
                both, pick, (((1,), (1,)), ((), ())), preferred_element_type=F32
            )
            dep[f] += sums[:cols] + sums[cols:]

    wide = 2 * move

    def deposit_stay(fields):
        def body(c, carry):
            deposit(stay[:, pl.ds(pl.multiple_of(c * wide, wide), wide)], fields)
            return carry

        lax.fori_loop(0, rows // wide, body, 0)

    def deposit_got(fields):
        for c in range(2):
            deposit(jnp.concatenate([got[2 * c], got[2 * c + 1]], axis=1), fields)

    dep[...] = jnp.zeros_like(dep)
    deposit_stay((4,))

    pl.semaphore_wait(barrier, len(everyone))
    sends = []
    for h in range(FACES):
        sends.append(
            pltpu.make_async_remote_copy(
                src_ref=bucket.at[h],
                dst_ref=got.at[h ^ 1],
                send_sem=bucket_send.at[h],
                recv_sem=bucket_recv.at[h ^ 1],
                device_id=near[h],
                device_id_type=MESH,
            )
        )
    for send in sends:
        send.start()
    deposit_stay((0, 1))
    for send in sends:
        send.wait()
    deposit_got((4,))
    loads[0].wait()
    total = ener[...] + dep[4]
    ener[...] = total
    press[...] = (ADIABATIC_INDEX - 1.0) * total
    for x in range(cells_x):
        side[0, pl.ds(x, 1)] = press[pl.ds(x * cells_y, 1)]
        side[1, pl.ds(x, 1)] = press[pl.ds(x * cells_y + cells_y - 1, 1)]
    outs = [
        pltpu.make_async_copy(ener, energy_out, store_sem.at[0]),
        pltpu.make_async_copy(got, arrived_out, store_sem.at[1]),
    ]
    for out in outs:
        out.start()
    faces = [
        press.at[pl.ds(0, cells_y)],
        press.at[pl.ds(cols - cells_y, cells_y)],
        side.at[0],
        side.at[1],
    ]
    sides = []
    for h in range(FACES):
        sides.append(
            pltpu.make_async_remote_copy(
                src_ref=faces[h],
                dst_ref=halo.at[h ^ 1],
                send_sem=halo_send.at[h],
                recv_sem=halo_recv.at[h ^ 1],
                device_id=near[h],
                device_id_type=MESH,
            )
        )
    for send in sides:
        send.start()
    deposit_got((0, 1, 2, 3))
    deposit_stay((2, 3))
    for load in loads[1:]:
        load.wait()
    for send in sides:
        send.wait()

    low_x = jnp.where(i > 0, halo[0], 0.0)
    high_x = jnp.where(i < nx - 1, halo[1], 0.0)
    low_y = jnp.where(j > 0, halo[2], 0.0)
    high_y = jnp.where(j < ny - 1, halo[3], 0.0)
    z = lane_iota((cells_y, depth))
    y = row_iota((cells_y, depth))
    fastest = jnp.zeros((cells_y, depth), F32)
    for x in range(cells_x):
        here = pl.ds(x * cells_y, cells_y)
        p = press[here]
        before = press[pl.ds((x - 1) * cells_y, cells_y)] if x else low_x
        after = press[pl.ds((x + 1) * cells_y, cells_y)] if x < cells_x - 1 else high_x
        below = jnp.where(y == 0, low_y[x : x + 1], pltpu.roll(p, 1, axis=0))
        above = jnp.where(y == cells_y - 1, high_y[x : x + 1], pltpu.roll(p, cells_y - 1, axis=0))
        under = jnp.where(z == 0, 0.0, pltpu.roll(p, 1, axis=1))
        over = jnp.where(z == depth - 1, 0.0, pltpu.roll(p, depth - 1, axis=1))
        rho = dens[here] + dep[0, here]
        dens[here] = rho
        wave = jnp.zeros_like(p)
        for k, (a, b) in enumerate(((before, after), (below, above), (under, over))):
            impulse = mom[k, here] + dep[k + 1, here] - KICK * (0.5 * (b - a))
            mom[k, here] = impulse
            wave = jnp.maximum(wave, jnp.abs(impulse / rho))
        wave = wave + jnp.sqrt(ADIABATIC_INDEX * p / rho)
        fastest = jnp.maximum(fastest, wave)
    late = [
        pltpu.make_async_copy(mom, momentum_out, store_sem.at[2]),
        pltpu.make_async_copy(dens, density_out, store_sem.at[3]),
    ]
    for out in late:
        out.start()
    top = jnp.max(fastest, axis=0, keepdims=True)
    top = jnp.maximum(top[:, :128], top[:, 128:])
    for phase, peers in enumerate((first, second)):
        best[phase] = top
        copies = []
        for q, peer in enumerate(peers):
            copies.append(
                pltpu.make_async_remote_copy(
                    src_ref=best.at[phase],
                    dst_ref=best_in.at[phase, q],
                    send_sem=best_send.at[phase, q],
                    recv_sem=best_recv.at[phase, q],
                    device_id=peer,
                    device_id_type=MESH,
                )
            )
        for copy in copies:
            copy.start()
        for copy in copies:
            copy.wait()
        for q in range(len(peers)):
            top = jnp.maximum(top, best_in[phase, q])
    step_out[...] = COURANT / jnp.broadcast_to(jnp.max(top, axis=1, keepdims=True), (1, 128))
    for out in outs + late:
        out.wait()


def on_device(density, momentum, energy, mass, velocity, temp, cell, count):
    cells_x, cells_y, depth = density.shape
    rows = mass.shape[0]
    move = rows // 16
    cols = cells_x * cells_y
    vmem = pl.BlockSpec(memory_space=VMEM)
    anyspace = pl.BlockSpec(memory_space=ANY)
    stay, bucket = pl.pallas_call(
        functools.partial(sort_kernel, cells_x, cells_y),
        name="sort_parcels",
        out_shape=(
            jax.ShapeDtypeStruct((8, rows), F32),
            jax.ShapeDtypeStruct((FACES, 8, move), F32),
        ),
        in_specs=[vmem] * 4 + [pl.BlockSpec(memory_space=pltpu.SMEM)],
        out_specs=(vmem, vmem),
        compiler_params=pltpu.CompilerParams(vmem_limit_bytes=48 * 2**20),
    )(mass.reshape(1, rows), velocity, temp.reshape(1, rows), cell, count)
    nx, ny = lax.axis_size("gx"), lax.axis_size("gy")
    field = jax.ShapeDtypeStruct((cols, depth), F32)
    dens, mom, ener, arrived, step = pl.pallas_call(
        functools.partial(main_kernel, nx, ny, cells_x, cells_y),
        name="deposit_and_push",
        out_shape=(
            field,
            jax.ShapeDtypeStruct((3, cols, depth), F32),
            field,
            jax.ShapeDtypeStruct((FACES, 8, move), F32),
            jax.ShapeDtypeStruct((1, 128), F32),
        ),
        in_specs=[vmem, vmem, anyspace, anyspace, anyspace],
        out_specs=(anyspace, anyspace, anyspace, anyspace, vmem),
        scratch_shapes=[
            VMEM((cols, depth), F32),
            VMEM((3, cols, depth), F32),
            VMEM((cols, depth), F32),
            VMEM((cols, depth), F32),
            VMEM((5, cols, depth), F32),
            VMEM((FACES, 8, move), F32),
            VMEM((2, cells_x, depth), F32),
            VMEM((FACES, cells_y, depth), F32),
            VMEM((2, 1, 128), F32),
            VMEM((2, 15, 1, 128), F32),
            pltpu.SemaphoreType.DMA((3,)),
            pltpu.SemaphoreType.DMA((4,)),
            pltpu.SemaphoreType.DMA((FACES,)),
            pltpu.SemaphoreType.DMA((FACES,)),
            pltpu.SemaphoreType.DMA((FACES,)),
            pltpu.SemaphoreType.DMA((FACES,)),
            pltpu.SemaphoreType.DMA((2, 15)),
            pltpu.SemaphoreType.DMA((2, 15)),
        ],
        compiler_params=pltpu.CompilerParams(
            vmem_limit_bytes=56 * 2**20, collective_id=0, has_side_effects=True
        ),
    )(
        stay,
        bucket,
        density.reshape(cols, depth),
        momentum.reshape(3, cols, depth),
        energy.reshape(cols, depth),
    )
    table = jnp.concatenate([stay] + [arrived[h] for h in range(FACES)], axis=1)
    return (
        dens.reshape(density.shape),
        mom.reshape(momentum.shape),
        ener.reshape(energy.shape),
        table[:5],
        table[5:].astype(jnp.int32),
        step[0, 0],
    )


def solution(mesh):
    both = ("gx", "gy")
    return jax.shard_map(
        on_device,
        mesh=mesh,
        in_specs=(
            P("gx", "gy", None),
            P(None, "gx", "gy", None),
            P("gx", "gy", None),
            P(both),
            P(None, both),
            P(both),
            P(None, both),
            P(both),
        ),
        out_specs=(
            P("gx", "gy", None),
            P(None, "gx", "gy", None),
            P("gx", "gy", None),
            P(None, both),
            P(None, both),
            P(),
        ),
        check_vma=False,
    )
```

```python
import functools

import jax
import jax.numpy as jnp
from jax import lax
from jax.experimental import pallas as pl
from jax.experimental.pallas import tpu as pltpu
from jax.sharding import PartitionSpec as P

ADIABATIC_INDEX = 1.4
KICK = 0.25
COURANT = 0.4
SHRINK = 0.5
FACES = 4
F32 = jnp.float32
BF16 = jnp.bfloat16
MESH = pl.DeviceIdType.MESH
VMEM = pltpu.VMEM
HBM = pltpu.HBM


def row_iota(shape):
    return lax.broadcasted_iota(jnp.int32, shape, 0)


def lane_iota(shape):
    return lax.broadcasted_iota(jnp.int32, shape, 1)


def pack_left(cells, shift, steps):
    width = cells.shape[1]
    for k in range(steps):
        step = 1 << k
        coming = pltpu.roll(cells, width - step, axis=1)
        coming_shift = pltpu.roll(shift, width - step, axis=1)
        take = (coming_shift & step) != 0
        leave = (shift & step) != 0
        cells = jnp.where(take, coming, cells)
        shift = jnp.where(take, coming_shift, jnp.where(leave, 0, shift))
    return cells, shift


def sort_parcels(
    cells_x, cells_y, anchor_x, anchor_y, mass, vel, temp, cell, count, stay_out, bucket_out
):
    rows = mass.shape[1]
    move = rows // 16
    chunk = 256
    chunks = rows // chunk
    live = lane_iota((1, rows)) < count[0]
    m, t = mass[...], temp[...]
    boiled = m * (1.0 / (1.0 + jnp.exp(4.0 - 2.0 * t)))
    left = m - SHRINK * boiled
    local_x = cell[0:1, :] - anchor_x
    local_y = cell[1:2, :] - anchor_y
    heading = jnp.where(
        local_x < 0,
        0,
        jnp.where(
            local_x >= cells_x, 1, jnp.where(local_y < 0, 2, jnp.where(local_y >= cells_y, 3, 4))
        ),
    )
    heading = jnp.where(live, heading, 5)
    record = jnp.concatenate([left, vel[...], t, cell[...].astype(F32)], axis=0)
    heads = jnp.broadcast_to(heading, (8, rows))
    stay_out[...] = jnp.where(heads == 4, record, 0.0)

    sub = row_iota((8, rows))
    mask = jnp.where((sub == heads) & (sub < 4), 1.0, 0.0)
    mask = jnp.where((sub == 4) & (heads < 4), 1.0, mask)
    stacked = jnp.concatenate(
        [mask[:, c * chunk : (c + 1) * chunk] for c in range(chunks)], axis=0
    ).astype(BF16)
    a, b = row_iota((chunk, chunk)), lane_iota((chunk, chunk))
    upper = jnp.where(a < b, 1.0, 0.0).astype(BF16)
    inside = jnp.dot(stacked, upper, preferred_element_type=F32)
    total = jnp.dot(stacked, jnp.ones((chunk, chunk), BF16), preferred_element_type=F32)
    n = 8 * chunks
    a, b = row_iota((n, n)), lane_iota((n, n))
    ahead = jnp.where(((a & 7) == (b & 7)) & (b < a), 1.0, 0.0).astype(BF16)
    before = jnp.dot(ahead, total.astype(BF16), preferred_element_type=F32)
    ranks = inside + before
    rank = jnp.concatenate([ranks[c * 8 : (c + 1) * 8] for c in range(chunks)], axis=1)
    counts = (before + total)[n - 8 : n, :128].astype(jnp.int32)

    own = jnp.sum(jnp.where(sub < 4, mask * rank, 0.0), axis=0, keepdims=True).astype(jnp.int32)
    overall = rank[4:5].astype(jnp.int32)
    moves = heading < 4
    shift = lane_iota((1, rows)) - overall
    target = heading * move + own
    shift = jnp.where(moves, shift + target * rows, 0)
    packed, key = pack_left(record, jnp.broadcast_to(shift, (8, rows)), rows.bit_length() - 1)

    wide = FACES * move
    packed = packed[:, :wide]
    slot = key[:, :wide] // rows
    place = lane_iota((8, wide))
    present = place < jnp.concatenate([counts[4:5]] * (wide // 128), axis=1)
    for h in range(FACES):
        mine = present & (slot // move == h)
        gap = jnp.where(mine, place - (slot - h * move), 0)
        out, _ = pack_left(packed, gap, wide.bit_length() - 1)
        full = jnp.concatenate([counts[h : h + 1]] * (move // 128), axis=1)
        bucket_out[h] = jnp.where(lane_iota((8, move)) < full, out[:, :move], 0.0)


def fused_kernel(
    nx,
    ny,
    cells_x,
    cells_y,
    mass,
    vel,
    temp,
    cell,
    count,
    density,
    momentum,
    energy,
    dens,
    mom,
    ener,
    state_out,
    cell_out,
    step_out,
    mass_in,
    vel_in,
    temp_in,
    cell_in,
    stay,
    bucket,
    press,
    dep,
    rim,
    got,
    side,
    halo,
    best,
    best_in,
    load_sem,
    bucket_send,
    bucket_recv,
    halo_send,
    halo_recv,
    best_send,
    best_recv,
):
    i, j = lax.axis_index("gx"), lax.axis_index("gy")
    cols = cells_x * cells_y
    depth = press.shape[1]
    rows = stay.shape[1]
    move = got.shape[2]
    up_x, down_x = lax.rem(i + 1, nx), lax.rem(i + nx - 1, nx)
    up_y, down_y = lax.rem(j + 1, ny), lax.rem(j + ny - 1, ny)
    near = [(down_x, j), (up_x, j), (i, down_y), (i, up_y)]
    half = ny // 2
    spot = lax.div(j, half) * nx + i
    lane = lax.rem(j, half)
    size_a, size_b = 2 * nx, half
    first = []
    for q in range(1, size_a):
        there = lax.rem(spot + q, size_a)
        first.append((lax.rem(there, nx), lax.div(there, nx) * half + lane))
    second = []
    for q in range(1, size_b):
        second.append((i, lax.div(j, half) * half + lax.rem(lane + q, size_b)))

    barrier = pltpu.get_barrier_semaphore()
    everyone = near + first + second
    for peer in everyone:
        pl.semaphore_signal(barrier, inc=1, device_id=peer, device_id_type=MESH)

    pairs = [
        (cell, cell_in),
        (mass, mass_in),
        (temp, temp_in),
        (vel, vel_in),
        (energy, ener),
        (density, dens),
        (momentum, mom),
    ]
    loads = [
        pltpu.make_async_copy(src, dst, load_sem.at[n]) for n, (src, dst) in enumerate(pairs)
    ]
    for load in loads:
        load.start()
    dep[...] = jnp.zeros_like(dep)
    for load in loads[:4]:
        load.wait()

    anchor_x, anchor_y = i * cells_x, j * cells_y
    sort_parcels(
        cells_x, cells_y, anchor_x, anchor_y, mass_in, vel_in, temp_in, cell_in, count, stay, bucket
    )
    state_out[:, :rows] = stay[:5]
    cell_out[:, :rows] = stay[5:].astype(jnp.int32)

    def terms(table, fields):
        v = table[1:4]
        t = table[4:5]
        boiled = table[0:1] / (0.5 + jnp.exp(4.0 - 2.0 * t))
        parts = []
        for f in fields:
            if f == 0:
                s = boiled
            elif f < 4:
                s = boiled * v[f - 1 : f]
            else:
                s = boiled * (t + 0.5 * jnp.sum(v * v, axis=0, keepdims=True))
            high = s.astype(BF16)
            low = (s - high.astype(F32)).astype(BF16)
            parts.append((high, low))
        return parts

    def picked(index, size):
        which = row_iota((size, index.shape[1])).astype(F32).astype(BF16)
        return which == index.astype(F32).astype(BF16)

    def sums_of(both, pick):
        return lax.dot_general(both, pick, (((1,), (1,)), ((), ())), preferred_element_type=F32)

    wide = 2 * move

    def deposit_stay(fields):
        def body(c, carry):
            table = stay[:, pl.ds(pl.multiple_of(c * wide, wide), wide)]
            parts = terms(table, fields)
            local_x = table[5:6].astype(jnp.int32) - anchor_x
            local_y = table[6:7].astype(jnp.int32) - anchor_y
            there = picked(local_x * cells_y + local_y, cols)
            pick = jnp.where(picked(table[7:8], depth), BF16(1), BF16(0))
            for f, halves in zip(fields, parts):
                both = jnp.concatenate([jnp.where(there, s, BF16(0)) for s in halves], axis=0)
                sums = sums_of(both, pick)
                dep[f] += sums[:cols] + sums[cols:]
            return carry

        lax.fori_loop(0, rows // wide, body, 0)

    def deposit_got():
        for b in range(FACES):
            table = got[b]
            parts = terms(table, range(5))
            if b < 2:
                along, length = table[6:7].astype(jnp.int32) - anchor_y, cells_y
            else:
                along, length = table[5:6].astype(jnp.int32) - anchor_x, cells_x
            there = picked(along, length)
            pick = jnp.where(picked(table[7:8], depth), BF16(1), BF16(0))
            both = jnp.concatenate(
                [jnp.where(there, s, BF16(0)) for halves in parts for s in halves], axis=0
            )
            sums = sums_of(both, pick)
            for f in range(5):
                o = 2 * f * length
                rim[b, f] = sums[o : o + length] + sums[o + length : o + 2 * length]
        for f in range(5):
            dep[f, :cells_y] += rim[0, f]
            dep[f, cols - cells_y :] += rim[1, f]

    pl.semaphore_wait(barrier, len(everyone))
    sends = []
    for h in range(FACES):
        sends.append(
            pltpu.make_async_remote_copy(
                src_ref=bucket.at[h],
                dst_ref=got.at[h ^ 1],
                send_sem=bucket_send.at[h],
                recv_sem=bucket_recv.at[h ^ 1],
                device_id=near[h],
                device_id_type=MESH,
            )
        )
    for send in sends:
        send.start()
    deposit_stay((4, 0, 1))
    for send in sends:
        send.wait()
    deposit_got()
    for b in range(FACES):
        here = pl.ds(rows + b * move, move)
        state_out[:, here] = got[b, :5]
        cell_out[:, here] = got[b, 5:].astype(jnp.int32)
    loads[4].wait()
    y = row_iota((cells_y, depth))
    for x in range(cells_x):
        here = pl.ds(x * cells_y, cells_y)
        edge = jnp.where(y == 0, rim[2, 4, x : x + 1], 0.0)
        edge += jnp.where(y == cells_y - 1, rim[3, 4, x : x + 1], 0.0)
        total = ener[here] + (dep[4, here] + edge)
        ener[here] = total
        p = (ADIABATIC_INDEX - 1.0) * total
        press[here] = p
        side[0, pl.ds(x, 1)] = p[:1]
        side[1, pl.ds(x, 1)] = p[cells_y - 1 :]
    faces = [
        press.at[pl.ds(0, cells_y)],
        press.at[pl.ds(cols - cells_y, cells_y)],
        side.at[0],
        side.at[1],
    ]
    sides = []
    for h in range(FACES):
        sides.append(
            pltpu.make_async_remote_copy(
                src_ref=faces[h],
                dst_ref=halo.at[h ^ 1],
                send_sem=halo_send.at[h],
                recv_sem=halo_recv.at[h ^ 1],
                device_id=near[h],
                device_id_type=MESH,
            )
        )
    for send in sides:
        send.start()
    deposit_stay((2, 3))
    for load in loads[5:]:
        load.wait()
    for send in sides:
        send.wait()

    low_x = jnp.where(i > 0, halo[0], 0.0)
    high_x = jnp.where(i < nx - 1, halo[1], 0.0)
    low_y = jnp.where(j > 0, halo[2], 0.0)
    high_y = jnp.where(j < ny - 1, halo[3], 0.0)
    z = lane_iota((cells_y, depth))
    fastest = jnp.zeros((cells_y, depth), F32)
    for x in range(cells_x):
        here = pl.ds(x * cells_y, cells_y)
        p = press[here]
        before = press[pl.ds((x - 1) * cells_y, cells_y)] if x else low_x
        after = press[pl.ds((x + 1) * cells_y, cells_y)] if x < cells_x - 1 else high_x
        below = jnp.where(y == 0, low_y[x : x + 1], pltpu.roll(p, 1, axis=0))
        above = jnp.where(y == cells_y - 1, high_y[x : x + 1], pltpu.roll(p, cells_y - 1, axis=0))
        under = jnp.where(z == 0, 0.0, pltpu.roll(p, 1, axis=1))
        over = jnp.where(z == depth - 1, 0.0, pltpu.roll(p, depth - 1, axis=1))

        def deposited(f):
            edge = jnp.where(y == 0, rim[2, f, x : x + 1], 0.0)
            edge += jnp.where(y == cells_y - 1, rim[3, f, x : x + 1], 0.0)
            return dep[f, here] + edge

        rho = dens[here] + deposited(0)
        dens[here] = rho
        speed = jnp.zeros_like(p)
        for k, (a, b) in enumerate(((before, after), (below, above), (under, over))):
            impulse = mom[k, here] + deposited(k + 1) - KICK * (0.5 * (b - a))
            mom[k, here] = impulse
            speed = jnp.maximum(speed, jnp.abs(impulse))
        wave = speed / rho + jnp.sqrt(ADIABATIC_INDEX * p / rho)
        fastest = jnp.maximum(fastest, wave)
    top = jnp.max(fastest, axis=0, keepdims=True)
    top = jnp.maximum(top[:, :128], top[:, 128:])
    for phase, peers in enumerate((first, second)):
        best[phase] = top
        copies = []
        for q, peer in enumerate(peers):
            copies.append(
                pltpu.make_async_remote_copy(
                    src_ref=best.at[phase],
                    dst_ref=best_in.at[phase, q],
                    send_sem=best_send.at[phase, q],
                    recv_sem=best_recv.at[phase, q],
                    device_id=peer,
                    device_id_type=MESH,
                )
            )
        for copy in copies:
            copy.start()
        for copy in copies:
            copy.wait()
        for q in range(len(peers)):
            top = jnp.maximum(top, best_in[phase, q])
    step_out[...] = COURANT / jnp.broadcast_to(jnp.max(top, axis=1, keepdims=True), (1, 128))


def on_device(density, momentum, energy, mass, velocity, temp, cell, count):
    cells_x, cells_y, depth = density.shape
    rows = mass.shape[0]
    move = rows // 16
    slots = rows + FACES * move
    cols = cells_x * cells_y
    vmem = pl.BlockSpec(memory_space=VMEM)
    far = pl.BlockSpec(memory_space=HBM)
    nx, ny = lax.axis_size("gx"), lax.axis_size("gy")
    field = jax.ShapeDtypeStruct((cols, depth), F32)
    dens, mom, ener, state, cells, step = pl.pallas_call(
        functools.partial(fused_kernel, nx, ny, cells_x, cells_y),
        name="spray_step",
        out_shape=(
            field,
            jax.ShapeDtypeStruct((3, cols, depth), F32),
            field,
            jax.ShapeDtypeStruct((5, slots), F32),
            jax.ShapeDtypeStruct((3, slots), jnp.int32),
            jax.ShapeDtypeStruct((1, 128), F32),
        ),
        in_specs=[far] * 4 + [pl.BlockSpec(memory_space=pltpu.SMEM)] + [far] * 3,
        out_specs=(vmem,) * 6,
        scratch_shapes=[
            VMEM((1, rows), F32),
            VMEM((3, rows), F32),
            VMEM((1, rows), F32),
            VMEM((3, rows), jnp.int32),
            VMEM((8, rows), F32),
            VMEM((FACES, 8, move), F32),
            VMEM((cols, depth), F32),
            VMEM((5, cols, depth), F32),
            VMEM((FACES, 5, cells_y, depth), F32),
            VMEM((FACES, 8, move), F32),
            VMEM((2, cells_x, depth), F32),
            VMEM((FACES, cells_y, depth), F32),
            VMEM((2, 1, 128), F32),
            VMEM((2, 15, 1, 128), F32),
            pltpu.SemaphoreType.DMA((7,)),
            pltpu.SemaphoreType.DMA((FACES,)),
            pltpu.SemaphoreType.DMA((FACES,)),
            pltpu.SemaphoreType.DMA((FACES,)),
            pltpu.SemaphoreType.DMA((FACES,)),
            pltpu.SemaphoreType.DMA((2, 15)),
            pltpu.SemaphoreType.DMA((2, 15)),
        ],
        compiler_params=pltpu.CompilerParams(
            vmem_limit_bytes=32 * 2**20, collective_id=0, has_side_effects=True
        ),
    )(
        mass.reshape(1, rows),
        velocity,
        temp.reshape(1, rows),
        cell,
        count,
        density.reshape(cols, depth),
        momentum.reshape(3, cols, depth),
        energy.reshape(cols, depth),
    )
    return (
        dens.reshape(density.shape),
        mom.reshape(momentum.shape),
        ener.reshape(energy.shape),
        state,
        cells,
        step[0, 0],
    )


def solution(mesh):
    both = ("gx", "gy")
    return jax.shard_map(
        on_device,
        mesh=mesh,
        in_specs=(
            P("gx", "gy", None),
            P(None, "gx", "gy", None),
            P("gx", "gy", None),
            P(both),
            P(None, both),
            P(both),
            P(None, both),
            P(both),
        ),
        out_specs=(
            P("gx", "gy", None),
            P(None, "gx", "gy", None),
            P("gx", "gy", None),
            P(None, both),
            P(None, both),
            P(),
        ),
        check_vma=False,
    )
```

```python
import functools

import jax
import jax.numpy as jnp
from jax import lax
from jax.experimental import pallas as pl
from jax.experimental.pallas import tpu as pltpu
from jax.sharding import PartitionSpec as P

ADIABATIC_INDEX = 1.4
KICK = 0.25
COURANT = 0.4
SHRINK = 0.5
FACES = 4
F32 = jnp.float32
BF16 = jnp.bfloat16
MESH = pl.DeviceIdType.MESH
VMEM = pltpu.VMEM
HBM = pltpu.HBM


def row_iota(shape):
    return lax.broadcasted_iota(jnp.int32, shape, 0)


def lane_iota(shape):
    return lax.broadcasted_iota(jnp.int32, shape, 1)


def pack_left(cells, shift, steps):
    width = cells.shape[1]
    for k in range(steps):
        step = 1 << k
        coming = pltpu.roll(cells, width - step, axis=1)
        coming_shift = pltpu.roll(shift, width - step, axis=1)
        take = (coming_shift & step) != 0
        leave = (shift & step) != 0
        cells = jnp.where(take, coming, cells)
        shift = jnp.where(take, coming_shift, jnp.where(leave, 0, shift))
    return cells, shift


def sort_parcels(
    cells_x, cells_y, anchor_x, anchor_y, mass, vel, temp, cell, count, stay_out, bucket_out
):
    rows = mass.shape[1]
    move = rows // 16
    chunk = 256
    chunks = rows // chunk
    live = lane_iota((1, rows)) < count[0]
    m, t = mass[...], temp[...]
    boiled = m * (1.0 / (1.0 + jnp.exp(4.0 - 2.0 * t)))
    left = m - SHRINK * boiled
    local_x = cell[0:1, :] - anchor_x
    local_y = cell[1:2, :] - anchor_y
    heading = jnp.where(
        local_x < 0,
        0,
        jnp.where(
            local_x >= cells_x, 1, jnp.where(local_y < 0, 2, jnp.where(local_y >= cells_y, 3, 4))
        ),
    )
    heading = jnp.where(live, heading, 5)
    record = jnp.concatenate([left, vel[...], t, cell[...].astype(F32)], axis=0)
    heads = jnp.broadcast_to(heading, (8, rows))
    stay_out[...] = jnp.where(heads == 4, record, 0.0)

    sub = row_iota((8, rows))
    mask = jnp.where((sub == heads) & (sub < 4), 1.0, 0.0)
    mask = jnp.where((sub == 4) & (heads < 4), 1.0, mask)
    stacked = jnp.concatenate(
        [mask[:, c * chunk : (c + 1) * chunk] for c in range(chunks)], axis=0
    ).astype(BF16)
    a, b = row_iota((chunk, chunk)), lane_iota((chunk, chunk))
    upper = jnp.where(a < b, 1.0, 0.0).astype(BF16)
    inside = jnp.dot(stacked, upper, preferred_element_type=F32)
    total = jnp.dot(stacked, jnp.ones((chunk, chunk), BF16), preferred_element_type=F32)
    n = 8 * chunks
    a, b = row_iota((n, n)), lane_iota((n, n))
    ahead = jnp.where(((a & 7) == (b & 7)) & (b < a), 1.0, 0.0).astype(BF16)
    before = jnp.dot(ahead, total.astype(BF16), preferred_element_type=F32)
    ranks = inside + before
    rank = jnp.concatenate([ranks[c * 8 : (c + 1) * 8] for c in range(chunks)], axis=1)
    counts = (before + total)[n - 8 : n, :128].astype(jnp.int32)

    own = jnp.sum(jnp.where(sub < 4, mask * rank, 0.0), axis=0, keepdims=True).astype(jnp.int32)
    overall = rank[4:5].astype(jnp.int32)
    moves = heading < 4
    shift = lane_iota((1, rows)) - overall
    target = heading * move + own
    shift = jnp.where(moves, shift + target * rows, 0)
    packed, key = pack_left(record, jnp.broadcast_to(shift, (8, rows)), rows.bit_length() - 1)

    wide = FACES * move
    packed = packed[:, :wide]
    slot = key[:, :wide] // rows
    place = lane_iota((8, wide))
    present = place < jnp.concatenate([counts[4:5]] * (wide // 128), axis=1)
    for h in range(FACES):
        mine = present & (slot // move == h)
        gap = jnp.where(mine, place - (slot - h * move), 0)
        out, _ = pack_left(packed, gap, wide.bit_length() - 1)
        full = jnp.concatenate([counts[h : h + 1]] * (move // 128), axis=1)
        bucket_out[h] = jnp.where(lane_iota((8, move)) < full, out[:, :move], 0.0)


def fused_kernel(
    nx,
    ny,
    cells_x,
    cells_y,
    mass,
    vel,
    temp,
    cell,
    count,
    density,
    momentum,
    energy,
    dens,
    mom,
    ener,
    state_out,
    cell_out,
    step_out,
    mass_in,
    vel_in,
    temp_in,
    cell_in,
    stay,
    bucket,
    press,
    dep,
    rim,
    got,
    side,
    halo,
    best,
    best_in,
    load_sem,
    bucket_send,
    bucket_recv,
    halo_send,
    halo_recv,
    best_send,
    best_recv,
):
    i, j = lax.axis_index("gx"), lax.axis_index("gy")
    cols = cells_x * cells_y
    depth = press.shape[1]
    rows = stay.shape[1]
    move = got.shape[2]
    up_x, down_x = lax.rem(i + 1, nx), lax.rem(i + nx - 1, nx)
    up_y, down_y = lax.rem(j + 1, ny), lax.rem(j + ny - 1, ny)
    near = [(down_x, j), (up_x, j), (i, down_y), (i, up_y)]
    half = ny // 2
    spot = lax.div(j, half) * nx + i
    lane = lax.rem(j, half)
    size_a, size_b = 2 * nx, half
    first = []
    for q in range(1, size_a):
        there = lax.rem(spot + q, size_a)
        first.append((lax.rem(there, nx), lax.div(there, nx) * half + lane))
    second = []
    for q in range(1, size_b):
        second.append((i, lax.div(j, half) * half + lax.rem(lane + q, size_b)))

    barrier = pltpu.get_barrier_semaphore()
    everyone = near + first + second
    for peer in everyone:
        pl.semaphore_signal(barrier, inc=1, device_id=peer, device_id_type=MESH)

    pairs = [
        (cell, cell_in),
        (mass, mass_in),
        (temp, temp_in),
        (vel, vel_in),
        (energy, ener),
        (density, dens),
        (momentum, mom),
    ]
    loads = [
        pltpu.make_async_copy(src, dst, load_sem.at[n]) for n, (src, dst) in enumerate(pairs)
    ]
    for load in loads:
        load.start()
    dep[...] = jnp.zeros_like(dep)
    for load in loads[:4]:
        load.wait()

    anchor_x, anchor_y = i * cells_x, j * cells_y
    sort_parcels(
        cells_x, cells_y, anchor_x, anchor_y, mass_in, vel_in, temp_in, cell_in, count, stay, bucket
    )
    state_out[:, :rows] = stay[:5]
    cell_out[:, :rows] = stay[5:].astype(jnp.int32)

    def terms(table, fields):
        v = table[1:4]
        t = table[4:5]
        boiled = table[0:1] / (0.5 + jnp.exp(4.0 - 2.0 * t))
        parts = []
        for f in fields:
            if f == 0:
                s = boiled
            elif f < 4:
                s = boiled * v[f - 1 : f]
            else:
                s = boiled * (t + 0.5 * jnp.sum(v * v, axis=0, keepdims=True))
            high = s.astype(BF16)
            low = (s - high.astype(F32)).astype(BF16)
            parts.append((high, low))
        return parts

    def picked(index, size):
        which = row_iota((size, index.shape[1])).astype(F32).astype(BF16)
        return which == index.astype(F32).astype(BF16)

    def sums_of(both, pick):
        return lax.dot_general(both, pick, (((1,), (1,)), ((), ())), preferred_element_type=F32)

    wide = 2 * move

    def deposit_stay(fields):
        def body(c, carry):
            table = stay[:, pl.ds(pl.multiple_of(c * wide, wide), wide)]
            parts = terms(table, fields)
            local_x = table[5:6].astype(jnp.int32) - anchor_x
            local_y = table[6:7].astype(jnp.int32) - anchor_y
            there = picked(local_x * cells_y + local_y, cols)
            pick = jnp.where(picked(table[7:8], depth), BF16(1), BF16(0))
            for f, halves in zip(fields, parts):
                both = jnp.concatenate([jnp.where(there, s, BF16(0)) for s in halves], axis=0)
                sums = sums_of(both, pick)
                dep[f] += sums[:cols] + sums[cols:]
            return carry

        lax.fori_loop(0, rows // wide, body, 0)

    def deposit_got():
        for b in range(FACES):
            table = got[b]
            parts = terms(table, range(5))
            if b < 2:
                along, length = table[6:7].astype(jnp.int32) - anchor_y, cells_y
            else:
                along, length = table[5:6].astype(jnp.int32) - anchor_x, cells_x
            there = picked(along, length)
            pick = jnp.where(picked(table[7:8], depth), BF16(1), BF16(0))
            both = jnp.concatenate(
                [jnp.where(there, s, BF16(0)) for halves in parts for s in halves], axis=0
            )
            sums = sums_of(both, pick)
            for f in range(5):
                o = 2 * f * length
                rim[b, f] = sums[o : o + length] + sums[o + length : o + 2 * length]
        for f in range(5):
            dep[f, :cells_y] += rim[0, f]
            dep[f, cols - cells_y :] += rim[1, f]

    pl.semaphore_wait(barrier, len(everyone))
    sends = []
    for h in range(FACES):
        sends.append(
            pltpu.make_async_remote_copy(
                src_ref=bucket.at[h],
                dst_ref=got.at[h ^ 1],
                send_sem=bucket_send.at[h],
                recv_sem=bucket_recv.at[h ^ 1],
                device_id=near[h],
                device_id_type=MESH,
            )
        )
    for send in sends:
        send.start()
    deposit_stay((4, 0, 1))
    for send in sends:
        send.wait()
    deposit_got()
    for b in range(FACES):
        here = pl.ds(rows + b * move, move)
        state_out[:, here] = got[b, :5]
        cell_out[:, here] = got[b, 5:].astype(jnp.int32)
    loads[4].wait()
    y = row_iota((cells_y, depth))
    for x in range(cells_x):
        here = pl.ds(x * cells_y, cells_y)
        edge = jnp.where(y == 0, rim[2, 4, x : x + 1], 0.0)
        edge += jnp.where(y == cells_y - 1, rim[3, 4, x : x + 1], 0.0)
        total = ener[here] + (dep[4, here] + edge)
        ener[here] = total
        p = (ADIABATIC_INDEX - 1.0) * total
        press[here] = p
        side[0, pl.ds(x, 1)] = p[:1]
        side[1, pl.ds(x, 1)] = p[cells_y - 1 :]
    faces = [
        press.at[pl.ds(0, cells_y)],
        press.at[pl.ds(cols - cells_y, cells_y)],
        side.at[0],
        side.at[1],
    ]
    sides = []
    for h in range(FACES):
        sides.append(
            pltpu.make_async_remote_copy(
                src_ref=faces[h],
                dst_ref=halo.at[h ^ 1],
                send_sem=halo_send.at[h],
                recv_sem=halo_recv.at[h ^ 1],
                device_id=near[h],
                device_id_type=MESH,
            )
        )
    for send in sides:
        send.start()
    deposit_stay((2, 3))
    for load in loads[5:]:
        load.wait()
    for send in sides:
        send.wait()

    low_x = jnp.where(i > 0, halo[0], 0.0)
    high_x = jnp.where(i < nx - 1, halo[1], 0.0)
    low_y = jnp.where(j > 0, halo[2], 0.0)
    high_y = jnp.where(j < ny - 1, halo[3], 0.0)
    z = lane_iota((cells_y, depth))
    fastest = jnp.zeros((cells_y, depth), F32)
    for x in range(cells_x):
        here = pl.ds(x * cells_y, cells_y)
        p = press[here]
        before = press[pl.ds((x - 1) * cells_y, cells_y)] if x else low_x
        after = press[pl.ds((x + 1) * cells_y, cells_y)] if x < cells_x - 1 else high_x
        below = jnp.where(y == 0, low_y[x : x + 1], pltpu.roll(p, 1, axis=0))
        above = jnp.where(y == cells_y - 1, high_y[x : x + 1], pltpu.roll(p, cells_y - 1, axis=0))
        under = jnp.where(z == 0, 0.0, pltpu.roll(p, 1, axis=1))
        over = jnp.where(z == depth - 1, 0.0, pltpu.roll(p, depth - 1, axis=1))

        def deposited(f):
            edge = jnp.where(y == 0, rim[2, f, x : x + 1], 0.0)
            edge += jnp.where(y == cells_y - 1, rim[3, f, x : x + 1], 0.0)
            return dep[f, here] + edge

        rho = dens[here] + deposited(0)
        dens[here] = rho
        speed = jnp.zeros_like(p)
        for k, (a, b) in enumerate(((before, after), (below, above), (under, over))):
            impulse = mom[k, here] + deposited(k + 1) - KICK * (0.5 * (b - a))
            mom[k, here] = impulse
            speed = jnp.maximum(speed, jnp.abs(impulse))
        wave = speed / rho + jnp.sqrt(ADIABATIC_INDEX * p / rho)
        fastest = jnp.maximum(fastest, wave)
    top = jnp.max(fastest, axis=0, keepdims=True)
    top = jnp.maximum(top[:, :128], top[:, 128:])
    for phase, peers in enumerate((first, second)):
        best[phase] = top
        copies = []
        for q, peer in enumerate(peers):
            copies.append(
                pltpu.make_async_remote_copy(
                    src_ref=best.at[phase],
                    dst_ref=best_in.at[phase, q],
                    send_sem=best_send.at[phase, q],
                    recv_sem=best_recv.at[phase, q],
                    device_id=peer,
                    device_id_type=MESH,
                )
            )
        for copy in copies:
            copy.start()
        for copy in copies:
            copy.wait()
        for q in range(len(peers)):
            top = jnp.maximum(top, best_in[phase, q])
    step_out[...] = COURANT / jnp.broadcast_to(jnp.max(top, axis=1, keepdims=True), (1, 128))


def write_kernel(*refs):
    sem = refs[-1]
    count = len(refs) // 2
    copies = [
        pltpu.make_async_copy(refs[n], refs[count + n], sem.at[n]) for n in range(count)
    ]
    for copy in copies:
        copy.start()
    for copy in copies:
        copy.wait()


def in_hbm(array):
    return pltpu.with_memory_space_constraint(array, HBM)


def on_device(density, momentum, energy, mass, velocity, temp, cell, count):
    cells_x, cells_y, depth = density.shape
    rows = mass.shape[0]
    move = rows // 16
    slots = rows + FACES * move
    cols = cells_x * cells_y
    vmem = pl.BlockSpec(memory_space=VMEM)
    far = pl.BlockSpec(memory_space=HBM)
    nx, ny = lax.axis_size("gx"), lax.axis_size("gy")
    field = jax.ShapeDtypeStruct((cols, depth), F32)
    dens, mom, ener, state, cells, step = pl.pallas_call(
        functools.partial(fused_kernel, nx, ny, cells_x, cells_y),
        name="spray_step",
        out_shape=(
            field,
            jax.ShapeDtypeStruct((3, cols, depth), F32),
            field,
            jax.ShapeDtypeStruct((5, slots), F32),
            jax.ShapeDtypeStruct((3, slots), jnp.int32),
            jax.ShapeDtypeStruct((1, 128), F32),
        ),
        in_specs=[far] * 4 + [pl.BlockSpec(memory_space=pltpu.SMEM)] + [far] * 3,
        out_specs=(vmem,) * 6,
        scratch_shapes=[
            VMEM((1, rows), F32),
            VMEM((3, rows), F32),
            VMEM((1, rows), F32),
            VMEM((3, rows), jnp.int32),
            VMEM((8, rows), F32),
            VMEM((FACES, 8, move), F32),
            VMEM((cols, depth), F32),
            VMEM((5, cols, depth), F32),
            VMEM((FACES, 5, cells_y, depth), F32),
            VMEM((FACES, 8, move), F32),
            VMEM((2, cells_x, depth), F32),
            VMEM((FACES, cells_y, depth), F32),
            VMEM((2, 1, 128), F32),
            VMEM((2, 15, 1, 128), F32),
            pltpu.SemaphoreType.DMA((7,)),
            pltpu.SemaphoreType.DMA((FACES,)),
            pltpu.SemaphoreType.DMA((FACES,)),
            pltpu.SemaphoreType.DMA((FACES,)),
            pltpu.SemaphoreType.DMA((FACES,)),
            pltpu.SemaphoreType.DMA((2, 15)),
            pltpu.SemaphoreType.DMA((2, 15)),
        ],
        compiler_params=pltpu.CompilerParams(
            vmem_limit_bytes=32 * 2**20, collective_id=0, has_side_effects=True
        ),
    )(
        in_hbm(mass.reshape(1, rows)),
        in_hbm(velocity),
        in_hbm(temp.reshape(1, rows)),
        in_hbm(cell),
        count,
        in_hbm(density.reshape(cols, depth)),
        in_hbm(momentum.reshape(3, cols, depth)),
        in_hbm(energy.reshape(cols, depth)),
    )
    results = (dens, mom, ener, state, cells, step)
    dens, mom, ener, state, cells, step = pl.pallas_call(
        write_kernel,
        name="write_results",
        out_shape=tuple(jax.ShapeDtypeStruct(r.shape, r.dtype) for r in results),
        in_specs=[vmem] * 6,
        out_specs=(far,) * 6,
        scratch_shapes=[pltpu.SemaphoreType.DMA((6,))],
        compiler_params=pltpu.CompilerParams(vmem_limit_bytes=2**20),
    )(*results)
    return (
        dens.reshape(density.shape),
        mom.reshape(momentum.shape),
        ener.reshape(energy.shape),
        state,
        cells,
        step[0, 0],
    )


def solution(mesh):
    both = ("gx", "gy")
    return jax.shard_map(
        on_device,
        mesh=mesh,
        in_specs=(
            P("gx", "gy", None),
            P(None, "gx", "gy", None),
            P("gx", "gy", None),
            P(both),
            P(None, both),
            P(both),
            P(None, both),
            P(both),
        ),
        out_specs=(
            P("gx", "gy", None),
            P(None, "gx", "gy", None),
            P("gx", "gy", None),
            P(None, both),
            P(None, both),
            P(),
        ),
        check_vma=False,
    )
```

```python
import functools

import jax
import jax.numpy as jnp
from jax import lax
from jax.experimental import pallas as pl
from jax.experimental.pallas import tpu as pltpu
from jax.sharding import PartitionSpec as P

ADIABATIC_INDEX = 1.4
KICK = 0.25
COURANT = 0.4
SHRINK = 0.5
FACES = 4
F32 = jnp.float32
BF16 = jnp.bfloat16
F8 = jnp.float8_e4m3fn
LOW_SCALE = 2048.0
MESH = pl.DeviceIdType.MESH
VMEM = pltpu.VMEM
HBM = pltpu.HBM


def row_iota(shape):
    return lax.broadcasted_iota(jnp.int32, shape, 0)


def lane_iota(shape):
    return lax.broadcasted_iota(jnp.int32, shape, 1)


def pack_left(cells, shift, steps):
    width = cells.shape[1]
    for k in range(steps):
        step = 1 << k
        coming = pltpu.roll(cells, width - step, axis=1)
        coming_shift = pltpu.roll(shift, width - step, axis=1)
        take = (coming_shift & step) != 0
        leave = (shift & step) != 0
        cells = jnp.where(take, coming, cells)
        shift = jnp.where(take, coming_shift, jnp.where(leave, 0, shift))
    return cells, shift


def sort_parcels(
    cells_x, cells_y, anchor_x, anchor_y, mass, vel, temp, cell, count, stay_out, bucket_out
):
    rows = mass.shape[1]
    move = rows // 16
    chunk = 256
    chunks = rows // chunk
    live = lane_iota((1, rows)) < count[0]
    m, t = mass[...], temp[...]
    boiled = m * (1.0 / (1.0 + jnp.exp(4.0 - 2.0 * t)))
    left = m - SHRINK * boiled
    local_x = cell[0:1, :] - anchor_x
    local_y = cell[1:2, :] - anchor_y
    heading = jnp.where(
        local_x < 0,
        0,
        jnp.where(
            local_x >= cells_x, 1, jnp.where(local_y < 0, 2, jnp.where(local_y >= cells_y, 3, 4))
        ),
    )
    heading = jnp.where(live, heading, 5)
    record = jnp.concatenate([left, vel[...], t, cell[...].astype(F32)], axis=0)
    heads = jnp.broadcast_to(heading, (8, rows))
    stay_out[...] = jnp.where(heads == 4, record, 0.0)

    sub = row_iota((8, rows))
    mask = jnp.where((sub == heads) & (sub < 4), 1.0, 0.0)
    mask = jnp.where((sub == 4) & (heads < 4), 1.0, mask)
    stacked = jnp.concatenate(
        [mask[:, c * chunk : (c + 1) * chunk] for c in range(chunks)], axis=0
    ).astype(BF16)
    a, b = row_iota((chunk, chunk)), lane_iota((chunk, chunk))
    upper = jnp.where(a < b, 1.0, 0.0).astype(BF16)
    inside = jnp.dot(stacked, upper, preferred_element_type=F32)
    total = jnp.dot(stacked, jnp.ones((chunk, chunk), BF16), preferred_element_type=F32)
    n = 8 * chunks
    a, b = row_iota((n, n)), lane_iota((n, n))
    ahead = jnp.where(((a & 7) == (b & 7)) & (b < a), 1.0, 0.0).astype(BF16)
    before = jnp.dot(ahead, total.astype(BF16), preferred_element_type=F32)
    ranks = inside + before
    rank = jnp.concatenate([ranks[c * 8 : (c + 1) * 8] for c in range(chunks)], axis=1)
    counts = (before + total)[n - 8 : n, :128].astype(jnp.int32)

    own = jnp.sum(jnp.where(sub < 4, mask * rank, 0.0), axis=0, keepdims=True).astype(jnp.int32)
    overall = rank[4:5].astype(jnp.int32)
    moves = heading < 4
    shift = lane_iota((1, rows)) - overall
    target = heading * move + own
    shift = jnp.where(moves, shift + target * rows, 0)
    packed, key = pack_left(record, jnp.broadcast_to(shift, (8, rows)), rows.bit_length() - 1)

    wide = FACES * move
    packed = packed[:, :wide]
    slot = key[:, :wide] // rows
    place = lane_iota((8, wide))
    present = place < jnp.concatenate([counts[4:5]] * (wide // 128), axis=1)
    for h in range(FACES):
        mine = present & (slot // move == h)
        gap = jnp.where(mine, place - (slot - h * move), 0)
        out, _ = pack_left(packed, gap, wide.bit_length() - 1)
        full = jnp.concatenate([counts[h : h + 1]] * (move // 128), axis=1)
        bucket_out[h] = jnp.where(lane_iota((8, move)) < full, out[:, :move], 0.0)


def fused_kernel(
    nx,
    ny,
    cells_x,
    cells_y,
    mass,
    vel,
    temp,
    cell,
    count,
    density,
    momentum,
    energy,
    dens,
    mom,
    ener,
    state_out,
    cell_out,
    step_out,
    mass_in,
    vel_in,
    temp_in,
    cell_in,
    stay,
    bucket,
    press,
    dep,
    rim,
    got,
    side,
    halo,
    best,
    best_in,
    load_sem,
    bucket_send,
    bucket_recv,
    halo_send,
    halo_recv,
    best_send,
    best_recv,
):
    i, j = lax.axis_index("gx"), lax.axis_index("gy")
    cols = cells_x * cells_y
    depth = press.shape[1]
    rows = stay.shape[1]
    move = got.shape[2]
    up_x, down_x = lax.rem(i + 1, nx), lax.rem(i + nx - 1, nx)
    up_y, down_y = lax.rem(j + 1, ny), lax.rem(j + ny - 1, ny)
    near = [(down_x, j), (up_x, j), (i, down_y), (i, up_y)]
    has = [i > 0, i < nx - 1, j > 0, j < ny - 1]
    half = ny // 2
    spot = lax.div(j, half) * nx + i
    lane = lax.rem(j, half)
    size_a, size_b = 2 * nx, half
    first = []
    for q in range(1, size_a):
        there = lax.rem(spot + q, size_a)
        first.append((lax.rem(there, nx), lax.div(there, nx) * half + lane))
    second = []
    for q in range(1, size_b):
        second.append((i, lax.div(j, half) * half + lax.rem(lane + q, size_b)))

    pairs = [
        (cell, cell_in),
        (mass, mass_in),
        (temp, temp_in),
        (vel, vel_in),
        (energy, ener),
        (density, dens),
        (momentum, mom),
    ]
    loads = [
        pltpu.make_async_copy(src, dst, load_sem.at[n]) for n, (src, dst) in enumerate(pairs)
    ]
    for load in loads:
        load.start()

    barrier = pltpu.get_barrier_semaphore()
    for peer in first + second:
        pl.semaphore_signal(barrier, inc=1, device_id=peer, device_id_type=MESH)
    for h in range(FACES):

        @pl.when(has[h])
        def _():
            pl.semaphore_signal(barrier, inc=1, device_id=near[h], device_id_type=MESH)

        @pl.when(jnp.logical_not(has[h]))
        def _():
            got[h] = jnp.zeros_like(got[h])
            halo[h] = jnp.zeros_like(halo[h])

    dep[...] = jnp.zeros_like(dep)
    for load in loads[:4]:
        load.wait()

    anchor_x, anchor_y = i * cells_x, j * cells_y
    sort_parcels(
        cells_x, cells_y, anchor_x, anchor_y, mass_in, vel_in, temp_in, cell_in, count, stay, bucket
    )
    def terms(table, fields, scale):
        v = table[1:4]
        t = table[4:5]
        boiled = table[0:1] / (0.5 + jnp.exp(4.0 - 2.0 * t))
        parts = []
        for f in fields:
            if f == 0:
                s = boiled
            elif f < 4:
                s = boiled * v[f - 1 : f]
            else:
                s = boiled * (t + 0.5 * jnp.sum(v * v, axis=0, keepdims=True))
            high = s.astype(BF16)
            low = ((s - high.astype(F32)) * scale).astype(BF16)
            parts.append((high, low))
        return parts

    def picked(index, size):
        which = row_iota((size, index.shape[1])).astype(F32).astype(BF16)
        return which == index.astype(F32).astype(BF16)

    def sums_of(both, pick):
        return lax.dot_general(both, pick, (((1,), (1,)), ((), ())), preferred_element_type=F32)

    wide = 4 * move

    def deposit_stay(fields):
        def body(c, carry):
            table = stay[:, pl.ds(pl.multiple_of(c * wide, wide), wide)]
            parts = terms(table, fields, LOW_SCALE)
            local_x = table[5:6].astype(jnp.int32) - anchor_x
            local_y = table[6:7].astype(jnp.int32) - anchor_y
            there = picked(local_x * cells_y + local_y, cols)
            pick = jnp.where(picked(table[7:8], depth), BF16(1), BF16(0))
            pick_low = pick.astype(F8)
            for f, (high, low) in zip(fields, parts):
                sums = sums_of(jnp.where(there, high, BF16(0)), pick)
                rest = sums_of(jnp.where(there, low, BF16(0)).astype(F8), pick_low)
                dep[f] += sums + rest * (1.0 / LOW_SCALE)
            return carry

        lax.fori_loop(0, rows // wide, body, 0)

    def arrivals(table, dim, fields):
        if dim == 0:
            along, length = table[6:7].astype(jnp.int32) - anchor_y, cells_y
        else:
            along, length = table[5:6].astype(jnp.int32) - anchor_x, cells_x
        there = picked(along, length)
        pick = jnp.where(picked(table[7:8], depth), BF16(1), BF16(0))
        parts = terms(table, fields, 1.0)
        both = jnp.concatenate(
            [jnp.where(there, s, BF16(0)) for halves in parts for s in halves], axis=0
        )
        sums = sums_of(both, pick)
        found = []
        for n in range(len(fields)):
            o = 2 * n * length
            found.append(sums[o : o + length] + sums[o + length : o + 2 * length])
        return found

    def start_all(copies, faces):
        for h in faces:
            pl.when(has[h])(copies[h].start)

    def wait_all(copies, faces):
        for h in faces:
            pl.when(has[h])(copies[h].wait_send)
            pl.when(has[h])(copies[h ^ 1].wait_recv)

    present = len(first) + len(second)
    for h in range(FACES):
        present = present + has[h].astype(jnp.int32)
    pl.semaphore_wait(barrier, present)
    sends = []
    for h in range(FACES):
        sends.append(
            pltpu.make_async_remote_copy(
                src_ref=bucket.at[h],
                dst_ref=got.at[h ^ 1],
                send_sem=bucket_send.at[h],
                recv_sem=bucket_recv.at[h ^ 1],
                device_id=near[h],
                device_id_type=MESH,
            )
        )
    start_all(sends, range(FACES))
    deposit_stay((4, 0, 1))
    wait_all(sends, (0, 1))
    for b, base in ((0, 0), (1, cols - cells_y)):
        for f, found in enumerate(arrivals(got[b], 0, range(5))):
            dep[f, base : base + cells_y] += found
    loads[4].wait()
    for x in range(cells_x):
        for n, y in enumerate((0, cells_y - 1)):
            here = pl.ds(x * cells_y + y, 1)
            side[n, pl.ds(x, 1)] = (ADIABATIC_INDEX - 1.0) * (ener[here] + dep[4, here])
    faces = [
        press.at[pl.ds(0, cells_y)],
        press.at[pl.ds(cols - cells_y, cells_y)],
        side.at[0],
        side.at[1],
    ]
    sides = []
    for h in range(FACES):
        sides.append(
            pltpu.make_async_remote_copy(
                src_ref=faces[h],
                dst_ref=halo.at[h ^ 1],
                send_sem=halo_send.at[h],
                recv_sem=halo_recv.at[h ^ 1],
                device_id=near[h],
                device_id_type=MESH,
            )
        )
    start_all(sides, (2, 3))
    wait_all(sends, (2, 3))
    for b in (2, 3):
        for f, found in enumerate(arrivals(got[b], 1, range(5))):
            rim[b - 2, f] = found
    y = row_iota((cells_y, depth))
    for x in range(cells_x):
        here = pl.ds(x * cells_y, cells_y)
        edge = jnp.where(y == 0, rim[0, 4, x : x + 1], 0.0)
        edge += jnp.where(y == cells_y - 1, rim[1, 4, x : x + 1], 0.0)
        total = ener[here] + (dep[4, here] + edge)
        ener[here] = total
        press[here] = (ADIABATIC_INDEX - 1.0) * total
    start_all(sides, (0, 1))
    gone = [arrivals(bucket[h], 1, (4,))[0] * (ADIABATIC_INDEX - 1.0) for h in (2, 3)]
    deposit_stay((2, 3))
    for load in loads[5:]:
        load.wait()
    wait_all(sides, range(FACES))

    low_x, high_x = halo[0], halo[1]
    low_y, high_y = halo[2] + gone[0], halo[3] + gone[1]
    z = lane_iota((cells_y, depth))
    fastest = jnp.zeros((cells_y, depth), F32)
    for x in range(cells_x):
        here = pl.ds(x * cells_y, cells_y)
        p = press[here]
        before = press[pl.ds((x - 1) * cells_y, cells_y)] if x else low_x
        after = press[pl.ds((x + 1) * cells_y, cells_y)] if x < cells_x - 1 else high_x
        below = jnp.where(y == 0, low_y[x : x + 1], pltpu.roll(p, 1, axis=0))
        above = jnp.where(y == cells_y - 1, high_y[x : x + 1], pltpu.roll(p, cells_y - 1, axis=0))
        under = jnp.where(z == 0, 0.0, pltpu.roll(p, 1, axis=1))
        over = jnp.where(z == depth - 1, 0.0, pltpu.roll(p, depth - 1, axis=1))

        def deposited(f):
            edge = jnp.where(y == 0, rim[0, f, x : x + 1], 0.0)
            edge += jnp.where(y == cells_y - 1, rim[1, f, x : x + 1], 0.0)
            return dep[f, here] + edge

        rho = dens[here] + deposited(0)
        dens[here] = rho
        speed = jnp.zeros_like(p)
        for k, (a, b) in enumerate(((before, after), (below, above), (under, over))):
            impulse = mom[k, here] + deposited(k + 1) - KICK * (0.5 * (b - a))
            mom[k, here] = impulse
            speed = jnp.maximum(speed, jnp.abs(impulse))
        wave = speed / rho + jnp.sqrt(ADIABATIC_INDEX * p / rho)
        fastest = jnp.maximum(fastest, wave)
    top = jnp.max(fastest, axis=0, keepdims=True)
    top = jnp.maximum(top[:, :128], top[:, 128:])
    for phase, peers in enumerate((first, second)):
        best[phase] = top
        copies = []
        for q, peer in enumerate(peers):
            copies.append(
                pltpu.make_async_remote_copy(
                    src_ref=best.at[phase],
                    dst_ref=best_in.at[phase, q],
                    send_sem=best_send.at[phase, q],
                    recv_sem=best_recv.at[phase, q],
                    device_id=peer,
                    device_id_type=MESH,
                )
            )
        for copy in copies:
            copy.start()
        if phase == 0:
            state_out[:, :rows] = stay[:5]
            cell_out[:, :rows] = stay[5:].astype(jnp.int32)
        else:
            for b in range(FACES):
                here = pl.ds(rows + b * move, move)
                state_out[:, here] = got[b, :5]
                cell_out[:, here] = got[b, 5:].astype(jnp.int32)
        for copy in copies:
            copy.wait()
        for q in range(len(peers)):
            top = jnp.maximum(top, best_in[phase, q])
    step_out[...] = COURANT / jnp.broadcast_to(jnp.max(top, axis=1, keepdims=True), (1, 128))


def write_kernel(*refs):
    sem = refs[-1]
    count = len(refs) // 2
    copies = [
        pltpu.make_async_copy(refs[n], refs[count + n], sem.at[n]) for n in range(count)
    ]
    for copy in copies:
        copy.start()
    for copy in copies:
        copy.wait()


def in_hbm(array):
    return pltpu.with_memory_space_constraint(array, HBM)


def on_device(density, momentum, energy, mass, velocity, temp, cell, count):
    cells_x, cells_y, depth = density.shape
    rows = mass.shape[0]
    move = rows // 16
    slots = rows + FACES * move
    cols = cells_x * cells_y
    vmem = pl.BlockSpec(memory_space=VMEM)
    far = pl.BlockSpec(memory_space=HBM)
    nx, ny = lax.axis_size("gx"), lax.axis_size("gy")
    field = jax.ShapeDtypeStruct((cols, depth), F32)
    dens, mom, ener, state, cells, step = pl.pallas_call(
        functools.partial(fused_kernel, nx, ny, cells_x, cells_y),
        name="spray_step",
        out_shape=(
            field,
            jax.ShapeDtypeStruct((3, cols, depth), F32),
            field,
            jax.ShapeDtypeStruct((5, slots), F32),
            jax.ShapeDtypeStruct((3, slots), jnp.int32),
            jax.ShapeDtypeStruct((1, 128), F32),
        ),
        in_specs=[far] * 4 + [pl.BlockSpec(memory_space=pltpu.SMEM)] + [far] * 3,
        out_specs=(vmem,) * 6,
        scratch_shapes=[
            VMEM((1, rows), F32),
            VMEM((3, rows), F32),
            VMEM((1, rows), F32),
            VMEM((3, rows), jnp.int32),
            VMEM((8, rows), F32),
            VMEM((FACES, 8, move), F32),
            VMEM((cols, depth), F32),
            VMEM((5, cols, depth), F32),
            VMEM((2, 5, cells_x, depth), F32),
            VMEM((FACES, 8, move), F32),
            VMEM((2, cells_x, depth), F32),
            VMEM((FACES, cells_y, depth), F32),
            VMEM((2, 1, 128), F32),
            VMEM((2, 15, 1, 128), F32),
            pltpu.SemaphoreType.DMA((7,)),
            pltpu.SemaphoreType.DMA((FACES,)),
            pltpu.SemaphoreType.DMA((FACES,)),
            pltpu.SemaphoreType.DMA((FACES,)),
            pltpu.SemaphoreType.DMA((FACES,)),
            pltpu.SemaphoreType.DMA((2, 15)),
            pltpu.SemaphoreType.DMA((2, 15)),
        ],
        compiler_params=pltpu.CompilerParams(
            vmem_limit_bytes=32 * 2**20, collective_id=0, has_side_effects=True
        ),
    )(
        in_hbm(mass.reshape(1, rows)),
        in_hbm(velocity),
        in_hbm(temp.reshape(1, rows)),
        in_hbm(cell),
        count,
        in_hbm(density.reshape(cols, depth)),
        in_hbm(momentum.reshape(3, cols, depth)),
        in_hbm(energy.reshape(cols, depth)),
    )
    results = (dens, mom, ener, state, cells, step)
    dens, mom, ener, state, cells, step = pl.pallas_call(
        write_kernel,
        name="write_results",
        out_shape=tuple(jax.ShapeDtypeStruct(r.shape, r.dtype) for r in results),
        in_specs=[vmem] * 6,
        out_specs=(far,) * 6,
        scratch_shapes=[pltpu.SemaphoreType.DMA((6,))],
        compiler_params=pltpu.CompilerParams(vmem_limit_bytes=2**20),
    )(*results)
    return (
        dens.reshape(density.shape),
        mom.reshape(momentum.shape),
        ener.reshape(energy.shape),
        state,
        cells,
        step[0, 0],
    )


def solution(mesh):
    both = ("gx", "gy")
    return jax.shard_map(
        on_device,
        mesh=mesh,
        in_specs=(
            P("gx", "gy", None),
            P(None, "gx", "gy", None),
            P("gx", "gy", None),
            P(both),
            P(None, both),
            P(both),
            P(None, both),
            P(both),
        ),
        out_specs=(
            P("gx", "gy", None),
            P(None, "gx", "gy", None),
            P("gx", "gy", None),
            P(None, both),
            P(None, both),
            P(),
        ),
        check_vma=False,
    )
```

```python
import functools

import jax
import jax.numpy as jnp
from jax import lax
from jax.experimental import pallas as pl
from jax.experimental.pallas import tpu as pltpu
from jax.sharding import PartitionSpec as P

ADIABATIC_INDEX = 1.4
KICK = 0.25
COURANT = 0.4
SHRINK = 0.5
FACES = 4
F32 = jnp.float32
BF16 = jnp.bfloat16
F8 = jnp.float8_e4m3fn
LOW_SCALE = 2048.0
MESH = pl.DeviceIdType.MESH
VMEM = pltpu.VMEM
HBM = pltpu.HBM


def row_iota(shape):
    return lax.broadcasted_iota(jnp.int32, shape, 0)


def lane_iota(shape):
    return lax.broadcasted_iota(jnp.int32, shape, 1)


def pack_left(cells, shift, steps):
    width = cells.shape[1]
    for k in range(steps):
        step = 1 << k
        coming = pltpu.roll(cells, width - step, axis=1)
        coming_shift = pltpu.roll(shift, width - step, axis=1)
        take = (coming_shift & step) != 0
        leave = (shift & step) != 0
        cells = jnp.where(take, coming, cells)
        shift = jnp.where(take, coming_shift, jnp.where(leave, 0, shift))
    return cells, shift


def sort_parcels(
    cells_x, cells_y, anchor_x, anchor_y, mass, vel, temp, cell, count, stay_out, bucket_out
):
    rows = mass.shape[1]
    move = rows // 16
    chunk = 256
    chunks = rows // chunk
    live = lane_iota((1, rows)) < count[0]
    m, t = mass[...], temp[...]
    boiled = m * (1.0 / (1.0 + jnp.exp(4.0 - 2.0 * t)))
    left = m - SHRINK * boiled
    local_x = cell[0:1, :] - anchor_x
    local_y = cell[1:2, :] - anchor_y
    heading = jnp.where(
        local_x < 0,
        0,
        jnp.where(
            local_x >= cells_x, 1, jnp.where(local_y < 0, 2, jnp.where(local_y >= cells_y, 3, 4))
        ),
    )
    heading = jnp.where(live, heading, 5)
    record = jnp.concatenate([left, vel[...], t, cell[...].astype(F32)], axis=0)
    heads = jnp.broadcast_to(heading, (8, rows))
    stay_out[...] = jnp.where(heads == 4, record, 0.0)

    sub = row_iota((8, rows))
    mask = jnp.where((sub == heads) & (sub < 4), 1.0, 0.0)
    mask = jnp.where((sub == 4) & (heads < 4), 1.0, mask)
    stacked = jnp.concatenate(
        [mask[:, c * chunk : (c + 1) * chunk] for c in range(chunks)], axis=0
    ).astype(BF16)
    a, b = row_iota((chunk, chunk)), lane_iota((chunk, chunk))
    upper = jnp.where(a < b, 1.0, 0.0).astype(BF16)
    inside = jnp.dot(stacked, upper, preferred_element_type=F32)
    total = jnp.dot(stacked, jnp.ones((chunk, chunk), BF16), preferred_element_type=F32)
    n = 8 * chunks
    a, b = row_iota((n, n)), lane_iota((n, n))
    ahead = jnp.where(((a & 7) == (b & 7)) & (b < a), 1.0, 0.0).astype(BF16)
    before = jnp.dot(ahead, total.astype(BF16), preferred_element_type=F32)
    ranks = inside + before
    rank = jnp.concatenate([ranks[c * 8 : (c + 1) * 8] for c in range(chunks)], axis=1)
    counts = (before + total)[n - 8 : n, :128].astype(jnp.int32)

    own = jnp.sum(jnp.where(sub < 4, mask * rank, 0.0), axis=0, keepdims=True).astype(jnp.int32)
    overall = rank[4:5].astype(jnp.int32)
    moves = heading < 4
    shift = lane_iota((1, rows)) - overall
    target = heading * move + own
    shift = jnp.where(moves, shift + target * rows, 0)
    packed, key = pack_left(record, jnp.broadcast_to(shift, (8, rows)), rows.bit_length() - 1)

    wide = FACES * move
    packed = packed[:, :wide]
    slot = key[:, :wide] // rows
    place = lane_iota((8, wide))
    present = place < jnp.concatenate([counts[4:5]] * (wide // 128), axis=1)
    for h in range(FACES):
        mine = present & (slot // move == h)
        gap = jnp.where(mine, place - (slot - h * move), 0)
        out, _ = pack_left(packed, gap, wide.bit_length() - 1)
        full = jnp.concatenate([counts[h : h + 1]] * (move // 128), axis=1)
        bucket_out[h] = jnp.where(lane_iota((8, move)) < full, out[:, :move], 0.0)


def fused_kernel(
    nx,
    ny,
    cells_x,
    cells_y,
    mass,
    vel,
    temp,
    cell,
    count,
    density,
    momentum,
    energy,
    dens,
    mom,
    ener,
    state_out,
    cell_out,
    step_out,
    mass_in,
    vel_in,
    temp_in,
    cell_in,
    stay,
    bucket,
    press,
    dep,
    rim,
    got,
    side,
    halo,
    best,
    best_in,
    load_sem,
    bucket_send,
    bucket_recv,
    halo_send,
    halo_recv,
    best_send,
    best_recv,
):
    i, j = lax.axis_index("gx"), lax.axis_index("gy")
    cols = cells_x * cells_y
    depth = press.shape[1]
    rows = stay.shape[1]
    move = got.shape[2]
    up_x, down_x = lax.rem(i + 1, nx), lax.rem(i + nx - 1, nx)
    up_y, down_y = lax.rem(j + 1, ny), lax.rem(j + ny - 1, ny)
    near = [(down_x, j), (up_x, j), (i, down_y), (i, up_y)]
    has = [i > 0, i < nx - 1, j > 0, j < ny - 1]
    half = ny // 2
    spot = lax.div(j, half) * nx + i
    lane = lax.rem(j, half)
    size_a, size_b = 2 * nx, half
    first = []
    for q in range(1, size_a):
        there = lax.rem(spot + q, size_a)
        first.append((lax.rem(there, nx), lax.div(there, nx) * half + lane))
    second = []
    for q in range(1, size_b):
        second.append((i, lax.div(j, half) * half + lax.rem(lane + q, size_b)))

    pairs = [
        (cell, cell_in),
        (mass, mass_in),
        (temp, temp_in),
        (vel, vel_in),
        (energy, ener),
        (density, dens),
        (momentum, mom),
    ]
    loads = [
        pltpu.make_async_copy(src, dst, load_sem.at[n]) for n, (src, dst) in enumerate(pairs)
    ]
    for load in loads:
        load.start()

    barrier = pltpu.get_barrier_semaphore()
    for peer in first + second:
        pl.semaphore_signal(barrier, inc=1, device_id=peer, device_id_type=MESH)
    for h in range(FACES):

        @pl.when(has[h])
        def _():
            pl.semaphore_signal(barrier, inc=1, device_id=near[h], device_id_type=MESH)

        @pl.when(jnp.logical_not(has[h]))
        def _():
            got[h] = jnp.zeros_like(got[h])
            halo[h] = jnp.zeros_like(halo[h])

    dep[...] = jnp.zeros_like(dep)
    for load in loads[:4]:
        load.wait()

    anchor_x, anchor_y = i * cells_x, j * cells_y
    def terms(table, fields, scale):
        v = table[1:4]
        t = table[4:5]
        boiled = table[0:1] / (0.5 + jnp.exp(4.0 - 2.0 * t))
        parts = []
        for f in fields:
            if f == 0:
                s = boiled
            elif f < 4:
                s = boiled * v[f - 1 : f]
            else:
                s = boiled * (t + 0.5 * jnp.sum(v * v, axis=0, keepdims=True))
            high = s.astype(BF16)
            low = ((s - high.astype(F32)) * scale).astype(BF16)
            parts.append((high, low))
        return parts

    def picked(index, size):
        which = row_iota((size, index.shape[1])).astype(F32).astype(BF16)
        return which == index.astype(F32).astype(BF16)

    def sums_of(both, pick):
        return lax.dot_general(both, pick, (((1,), (1,)), ((), ())), preferred_element_type=F32)

    def deposit_stay(fields, wide):
        def body(start):
            table = stay[:, pl.ds(start, wide)]
            parts = terms(table, fields, LOW_SCALE)
            local_x = table[5:6].astype(jnp.int32) - anchor_x
            local_y = table[6:7].astype(jnp.int32) - anchor_y
            there = picked(local_x * cells_y + local_y, cols)
            pick = jnp.where(picked(table[7:8], depth), BF16(1), BF16(0))
            pick_low = pick.astype(F8)
            for f, (high, low) in zip(fields, parts):
                sums = sums_of(jnp.where(there, high, BF16(0)), pick)
                rest = sums_of(jnp.where(there, low, BF16(0)).astype(F8), pick_low)
                dep[f] += sums + rest * (1.0 / LOW_SCALE)

        return body

    def deposit_loop(fields):
        wide = 8 * move
        body = deposit_stay(fields, wide)

        def step(c, carry):
            body(pl.multiple_of(c * wide, wide))
            return carry

        lax.fori_loop(0, rows // wide, step, 0)

    def arrivals(table, dim, fields):
        if dim == 0:
            along, length = table[6:7].astype(jnp.int32) - anchor_y, cells_y
        else:
            along, length = table[5:6].astype(jnp.int32) - anchor_x, cells_x
        there = picked(along, length)
        pick = jnp.where(picked(table[7:8], depth), BF16(1), BF16(0))
        parts = terms(table, fields, 1.0)
        both = jnp.concatenate(
            [jnp.where(there, s, BF16(0)) for halves in parts for s in halves], axis=0
        )
        sums = sums_of(both, pick)
        found = []
        for n in range(len(fields)):
            o = 2 * n * length
            found.append(sums[o : o + length] + sums[o + length : o + 2 * length])
        return found

    def start_all(copies, faces):
        for h in faces:
            pl.when(has[h])(copies[h].start)

    def wait_all(copies, faces):
        for h in faces:
            pl.when(has[h])(copies[h].wait_send)
            pl.when(has[h])(copies[h ^ 1].wait_recv)

    sort_parcels(
        cells_x, cells_y, anchor_x, anchor_y, mass_in, vel_in, temp_in, cell_in, count, stay, bucket
    )
    wide = rows
    for start in range(0, rows, wide):
        deposit_stay((4,), wide)(start)

    present = len(first) + len(second)
    for h in range(FACES):
        present = present + has[h].astype(jnp.int32)
    pl.semaphore_wait(barrier, present)
    sends = []
    for h in range(FACES):
        sends.append(
            pltpu.make_async_remote_copy(
                src_ref=bucket.at[h],
                dst_ref=got.at[h ^ 1],
                send_sem=bucket_send.at[h],
                recv_sem=bucket_recv.at[h ^ 1],
                device_id=near[h],
                device_id_type=MESH,
            )
        )
    start_all(sends, range(FACES))
    deposit_loop((0, 1,))
    wait_all(sends, (0, 1))
    for b, base in ((0, 0), (1, cols - cells_y)):
        for f, found in enumerate(arrivals(got[b], 0, range(5))):
            dep[f, base : base + cells_y] += found
    loads[4].wait()
    for x in range(cells_x):
        for n, y in enumerate((0, cells_y - 1)):
            here = pl.ds(x * cells_y + y, 1)
            side[n, pl.ds(x, 1)] = (ADIABATIC_INDEX - 1.0) * (ener[here] + dep[4, here])
    faces = [
        press.at[pl.ds(0, cells_y)],
        press.at[pl.ds(cols - cells_y, cells_y)],
        side.at[0],
        side.at[1],
    ]
    sides = []
    for h in range(FACES):
        sides.append(
            pltpu.make_async_remote_copy(
                src_ref=faces[h],
                dst_ref=halo.at[h ^ 1],
                send_sem=halo_send.at[h],
                recv_sem=halo_recv.at[h ^ 1],
                device_id=near[h],
                device_id_type=MESH,
            )
        )
    start_all(sides, (2, 3))
    wait_all(sends, (2, 3))
    for b in (2, 3):
        for f, found in enumerate(arrivals(got[b], 1, range(5))):
            rim[b - 2, f] = found
    y = row_iota((cells_y, depth))
    for x in range(cells_x):
        here = pl.ds(x * cells_y, cells_y)
        edge = jnp.where(y == 0, rim[0, 4, x : x + 1], 0.0)
        edge += jnp.where(y == cells_y - 1, rim[1, 4, x : x + 1], 0.0)
        total = ener[here] + (dep[4, here] + edge)
        ener[here] = total
        press[here] = (ADIABATIC_INDEX - 1.0) * total
    start_all(sides, (0, 1))
    gone = [arrivals(bucket[h], 1, (4,))[0] * (ADIABATIC_INDEX - 1.0) for h in (2, 3)]
    deposit_loop((2, 3))
    for load in loads[5:]:
        load.wait()
    wait_all(sides, range(FACES))

    low_x, high_x = halo[0], halo[1]
    low_y, high_y = halo[2] + gone[0], halo[3] + gone[1]
    z = lane_iota((cells_y, depth))
    fastest = jnp.zeros((cells_y, depth), F32)
    for x in range(cells_x):
        here = pl.ds(x * cells_y, cells_y)
        p = press[here]
        before = press[pl.ds((x - 1) * cells_y, cells_y)] if x else low_x
        after = press[pl.ds((x + 1) * cells_y, cells_y)] if x < cells_x - 1 else high_x
        below = jnp.where(y == 0, low_y[x : x + 1], pltpu.roll(p, 1, axis=0))
        above = jnp.where(y == cells_y - 1, high_y[x : x + 1], pltpu.roll(p, cells_y - 1, axis=0))
        under = jnp.where(z == 0, 0.0, pltpu.roll(p, 1, axis=1))
        over = jnp.where(z == depth - 1, 0.0, pltpu.roll(p, depth - 1, axis=1))

        def deposited(f):
            edge = jnp.where(y == 0, rim[0, f, x : x + 1], 0.0)
            edge += jnp.where(y == cells_y - 1, rim[1, f, x : x + 1], 0.0)
            return dep[f, here] + edge

        rho = dens[here] + deposited(0)
        dens[here] = rho
        speed = jnp.zeros_like(p)
        for k, (a, b) in enumerate(((before, after), (below, above), (under, over))):
            impulse = mom[k, here] + deposited(k + 1) - KICK * (0.5 * (b - a))
            mom[k, here] = impulse
            speed = jnp.maximum(speed, jnp.abs(impulse))
        wave = speed / rho + jnp.sqrt(ADIABATIC_INDEX * p / rho)
        fastest = jnp.maximum(fastest, wave)
    top = jnp.max(fastest, axis=0, keepdims=True)
    top = jnp.maximum(top[:, :128], top[:, 128:])
    for phase, peers in enumerate((first, second)):
        best[phase] = top
        copies = []
        for q, peer in enumerate(peers):
            copies.append(
                pltpu.make_async_remote_copy(
                    src_ref=best.at[phase],
                    dst_ref=best_in.at[phase, q],
                    send_sem=best_send.at[phase, q],
                    recv_sem=best_recv.at[phase, q],
                    device_id=peer,
                    device_id_type=MESH,
                )
            )
        for copy in copies:
            copy.start()
        if phase == 0:
            state_out[:, :rows] = stay[:5]
            cell_out[:, :rows] = stay[5:].astype(jnp.int32)
        else:
            for b in range(FACES):
                here = pl.ds(rows + b * move, move)
                state_out[:, here] = got[b, :5]
                cell_out[:, here] = got[b, 5:].astype(jnp.int32)
        for copy in copies:
            copy.wait()
        for q in range(len(peers)):
            top = jnp.maximum(top, best_in[phase, q])
    step_out[...] = COURANT / jnp.broadcast_to(jnp.max(top, axis=1, keepdims=True), (1, 128))


def write_kernel(*refs):
    sem = refs[-1]
    count = len(refs) // 2
    copies = [
        pltpu.make_async_copy(refs[n], refs[count + n], sem.at[n]) for n in range(count)
    ]
    for copy in copies:
        copy.start()
    for copy in copies:
        copy.wait()


def in_hbm(array):
    return pltpu.with_memory_space_constraint(array, HBM)


def on_device(density, momentum, energy, mass, velocity, temp, cell, count):
    cells_x, cells_y, depth = density.shape
    rows = mass.shape[0]
    move = rows // 16
    slots = rows + FACES * move
    cols = cells_x * cells_y
    vmem = pl.BlockSpec(memory_space=VMEM)
    far = pl.BlockSpec(memory_space=HBM)
    nx, ny = lax.axis_size("gx"), lax.axis_size("gy")
    field = jax.ShapeDtypeStruct((cols, depth), F32)
    dens, mom, ener, state, cells, step = pl.pallas_call(
        functools.partial(fused_kernel, nx, ny, cells_x, cells_y),
        name="spray_step",
        out_shape=(
            field,
            jax.ShapeDtypeStruct((3, cols, depth), F32),
            field,
            jax.ShapeDtypeStruct((5, slots), F32),
            jax.ShapeDtypeStruct((3, slots), jnp.int32),
            jax.ShapeDtypeStruct((1, 128), F32),
        ),
        in_specs=[far] * 4 + [pl.BlockSpec(memory_space=pltpu.SMEM)] + [far] * 3,
        out_specs=(vmem,) * 6,
        scratch_shapes=[
            VMEM((1, rows), F32),
            VMEM((3, rows), F32),
            VMEM((1, rows), F32),
            VMEM((3, rows), jnp.int32),
            VMEM((8, rows), F32),
            VMEM((FACES, 8, move), F32),
            VMEM((cols, depth), F32),
            VMEM((5, cols, depth), F32),
            VMEM((2, 5, cells_x, depth), F32),
            VMEM((FACES, 8, move), F32),
            VMEM((2, cells_x, depth), F32),
            VMEM((FACES, cells_y, depth), F32),
            VMEM((2, 1, 128), F32),
            VMEM((2, 15, 1, 128), F32),
            pltpu.SemaphoreType.DMA((7,)),
            pltpu.SemaphoreType.DMA((FACES,)),
            pltpu.SemaphoreType.DMA((FACES,)),
            pltpu.SemaphoreType.DMA((FACES,)),
            pltpu.SemaphoreType.DMA((FACES,)),
            pltpu.SemaphoreType.DMA((2, 15)),
            pltpu.SemaphoreType.DMA((2, 15)),
        ],
        compiler_params=pltpu.CompilerParams(
            vmem_limit_bytes=32 * 2**20, collective_id=0, has_side_effects=True
        ),
    )(
        in_hbm(mass.reshape(1, rows)),
        in_hbm(velocity),
        in_hbm(temp.reshape(1, rows)),
        in_hbm(cell),
        count,
        in_hbm(density.reshape(cols, depth)),
        in_hbm(momentum.reshape(3, cols, depth)),
        in_hbm(energy.reshape(cols, depth)),
    )
    results = (dens, mom, ener, state, cells, step)
    dens, mom, ener, state, cells, step = pl.pallas_call(
        write_kernel,
        name="write_results",
        out_shape=tuple(jax.ShapeDtypeStruct(r.shape, r.dtype) for r in results),
        in_specs=[vmem] * 6,
        out_specs=(far,) * 6,
        scratch_shapes=[pltpu.SemaphoreType.DMA((6,))],
        compiler_params=pltpu.CompilerParams(vmem_limit_bytes=2**20),
    )(*results)
    return (
        dens.reshape(density.shape),
        mom.reshape(momentum.shape),
        ener.reshape(energy.shape),
        state,
        cells,
        step[0, 0],
    )


def solution(mesh):
    both = ("gx", "gy")
    return jax.shard_map(
        on_device,
        mesh=mesh,
        in_specs=(
            P("gx", "gy", None),
            P(None, "gx", "gy", None),
            P("gx", "gy", None),
            P(both),
            P(None, both),
            P(both),
            P(None, both),
            P(both),
        ),
        out_specs=(
            P("gx", "gy", None),
            P(None, "gx", "gy", None),
            P("gx", "gy", None),
            P(None, both),
            P(None, both),
            P(),
        ),
        check_vma=False,
    )
```

```python
import functools

import jax
import jax.numpy as jnp
from jax import lax
from jax.experimental import pallas as pl
from jax.experimental.pallas import tpu as pltpu
from jax.sharding import PartitionSpec as P

ADIABATIC_INDEX = 1.4
KICK = 0.25
COURANT = 0.4
SHRINK = 0.5
FACES = 4
F32 = jnp.float32
BF16 = jnp.bfloat16
F8 = jnp.float8_e4m3fn
LOW_SCALE = 2048.0
MESH = pl.DeviceIdType.MESH
VMEM = pltpu.VMEM
HBM = pltpu.HBM


def row_iota(shape):
    return lax.broadcasted_iota(jnp.int32, shape, 0)


def lane_iota(shape):
    return lax.broadcasted_iota(jnp.int32, shape, 1)


def folded(row, parts):
    width = row.shape[1] // parts
    pieces = [
        row[r : r + 1, k * width : (k + 1) * width]
        for r in range(row.shape[0])
        for k in range(parts)
    ]
    return jnp.concatenate(pieces, axis=0)


def folded_left(fold, step):
    width = fold.shape[1]
    if step >= width:
        return pltpu.roll(fold, 8 - step // width, axis=0)
    near = pltpu.roll(fold, width - step, axis=1)
    return jnp.where(lane_iota(fold.shape) >= width - step, pltpu.roll(near, 7, axis=0), near)


def pack_left(cells, shift, steps):
    width = cells.shape[1]
    part = shift.shape[1]
    for k in range(steps):
        step = 1 << k
        coming_shift = folded_left(shift, step)
        take = coming_shift & step
        shift = jnp.where(take != 0, coming_shift, jnp.where((shift & step) != 0, 0, shift))
        spread = jnp.concatenate(
            [jnp.broadcast_to(take[r : r + 1], (8, part)) for r in range(8)], axis=1
        )
        cells = jnp.where(spread != 0, pltpu.roll(cells, width - step, axis=1), cells)
    return cells, shift


def sort_parcels(
    cells_x, cells_y, anchor_x, anchor_y, mass, vel, temp, cell, count, stay_out, bucket_out
):
    rows = mass.shape[1]
    move = rows // 16
    chunk = 256
    chunks = rows // chunk
    live = lane_iota((1, rows)) < count[0]
    m, t = mass[...], temp[...]
    boiled = m * (1.0 / (1.0 + jnp.exp(4.0 - 2.0 * t)))
    left = m - SHRINK * boiled
    local_x = cell[0:1, :] - anchor_x
    local_y = cell[1:2, :] - anchor_y
    heading = jnp.where(
        local_x < 0,
        0,
        jnp.where(
            local_x >= cells_x, 1, jnp.where(local_y < 0, 2, jnp.where(local_y >= cells_y, 3, 4))
        ),
    )
    heading = jnp.where(live, heading, 5)
    record = jnp.concatenate([left, vel[...], t, cell[...].astype(F32)], axis=0)
    heads = jnp.broadcast_to(heading, (8, rows))
    stay_out[...] = jnp.where(heads == 4, record, 0.0)

    sub = row_iota((8, rows))
    mask = jnp.where((sub == heads) & (sub < 4), 1.0, 0.0)
    mask = jnp.where((sub == 4) & (heads < 4), 1.0, mask)
    stacked = jnp.concatenate(
        [mask[:, c * chunk : (c + 1) * chunk] for c in range(chunks)], axis=0
    ).astype(BF16)
    a, b = row_iota((chunk, chunk)), lane_iota((chunk, chunk))
    upper = jnp.where(a < b, 1.0, 0.0).astype(BF16)
    inside = jnp.dot(stacked, upper, preferred_element_type=F32)
    total = jnp.dot(stacked, jnp.ones((chunk, chunk), BF16), preferred_element_type=F32)
    n = 8 * chunks
    a, b = row_iota((n, n)), lane_iota((n, n))
    ahead = jnp.where(((a & 7) == (b & 7)) & (b < a), 1.0, 0.0).astype(BF16)
    before = jnp.dot(ahead, total.astype(BF16), preferred_element_type=F32)
    ranks = inside + before
    rank = jnp.concatenate([ranks[c * 8 : (c + 1) * 8] for c in range(chunks)], axis=1)
    counts = (before + total)[n - 8 : n, :128].astype(jnp.int32)

    own = jnp.sum(jnp.where(sub < 4, mask * rank, 0.0), axis=0, keepdims=True).astype(jnp.int32)
    overall = rank[4:5].astype(jnp.int32)
    moves = heading < 4
    shift = lane_iota((1, rows)) - overall
    target = heading * move + own
    shift = jnp.where(moves, shift + target * rows, 0)
    packed, key = pack_left(record, folded(shift, 8), rows.bit_length() - 1)

    wide = FACES * move
    eighth = wide // 8
    packed = packed[:, :wide]
    lead = wide * 8 // rows
    slot = folded(key[:lead], 8 // lead) // rows
    place = row_iota((8, eighth)) * eighth + lane_iota((8, eighth))
    movers = jnp.concatenate([counts[4:5]] * (eighth // 128), axis=1)
    present = place < jnp.broadcast_to(movers, (8, eighth))
    for h in range(FACES):
        mine = present & (slot // move == h)
        gap = jnp.where(mine, place - (slot - h * move), 0)
        out, _ = pack_left(packed, gap, wide.bit_length() - 1)
        full = jnp.concatenate([counts[h : h + 1]] * (move // 128), axis=1)
        bucket_out[h] = jnp.where(lane_iota((8, move)) < full, out[:, :move], 0.0)


def fused_kernel(
    nx,
    ny,
    cells_x,
    cells_y,
    mass,
    vel,
    temp,
    cell,
    count,
    density,
    momentum,
    energy,
    dens,
    mom,
    ener,
    state_out,
    cell_out,
    step_out,
    mass_in,
    vel_in,
    temp_in,
    cell_in,
    stay,
    bucket,
    press,
    dep,
    rim,
    got,
    side,
    halo,
    best,
    best_in,
    load_sem,
    bucket_send,
    bucket_recv,
    halo_send,
    halo_recv,
    best_send,
    best_recv,
):
    i, j = lax.axis_index("gx"), lax.axis_index("gy")
    cols = cells_x * cells_y
    depth = press.shape[1]
    rows = stay.shape[1]
    move = got.shape[2]
    up_x, down_x = lax.rem(i + 1, nx), lax.rem(i + nx - 1, nx)
    up_y, down_y = lax.rem(j + 1, ny), lax.rem(j + ny - 1, ny)
    near = [(down_x, j), (up_x, j), (i, down_y), (i, up_y)]
    has = [i > 0, i < nx - 1, j > 0, j < ny - 1]
    half = ny // 2
    spot = lax.div(j, half) * nx + i
    lane = lax.rem(j, half)
    size_a, size_b = 2 * nx, half
    first = []
    for q in range(1, size_a):
        there = lax.rem(spot + q, size_a)
        first.append((lax.rem(there, nx), lax.div(there, nx) * half + lane))
    second = []
    for q in range(1, size_b):
        second.append((i, lax.div(j, half) * half + lax.rem(lane + q, size_b)))

    pairs = [
        (cell, cell_in),
        (mass, mass_in),
        (temp, temp_in),
        (vel, vel_in),
        (energy, ener),
        (density, dens),
        (momentum, mom),
    ]
    loads = [
        pltpu.make_async_copy(src, dst, load_sem.at[n]) for n, (src, dst) in enumerate(pairs)
    ]
    for load in loads:
        load.start()

    barrier = pltpu.get_barrier_semaphore()
    for peer in first + second:
        pl.semaphore_signal(barrier, inc=1, device_id=peer, device_id_type=MESH)
    for h in range(FACES):

        @pl.when(has[h])
        def _():
            pl.semaphore_signal(barrier, inc=1, device_id=near[h], device_id_type=MESH)

        @pl.when(jnp.logical_not(has[h]))
        def _():
            got[h] = jnp.zeros_like(got[h])
            halo[h] = jnp.zeros_like(halo[h])

    dep[...] = jnp.zeros_like(dep)
    for load in loads[:4]:
        load.wait()

    anchor_x, anchor_y = i * cells_x, j * cells_y
    def terms(table, fields, scale):
        v = table[1:4]
        t = table[4:5]
        boiled = table[0:1] / (0.5 + jnp.exp(4.0 - 2.0 * t))
        parts = []
        for f in fields:
            if f == 0:
                s = boiled
            elif f < 4:
                s = boiled * v[f - 1 : f]
            else:
                s = boiled * (t + 0.5 * jnp.sum(v * v, axis=0, keepdims=True))
            high = s.astype(BF16)
            low = ((s - high.astype(F32)) * scale).astype(BF16)
            parts.append((high, low))
        return parts

    def picked(index, size):
        which = row_iota((size, index.shape[1])).astype(F32).astype(BF16)
        return which == index.astype(F32).astype(BF16)

    def sums_of(both, pick):
        return lax.dot_general(both, pick, (((1,), (1,)), ((), ())), preferred_element_type=F32)

    def deposit_stay(fields, wide):
        def body(start):
            table = stay[:, pl.ds(start, wide)]
            parts = terms(table, fields, LOW_SCALE)
            local_x = table[5:6].astype(jnp.int32) - anchor_x
            local_y = table[6:7].astype(jnp.int32) - anchor_y
            there = picked(local_x * cells_y + local_y, cols)
            pick = jnp.where(picked(table[7:8], depth), BF16(1), BF16(0))
            pick_low = pick.astype(F8)
            for f, (high, low) in zip(fields, parts):
                sums = sums_of(jnp.where(there, high, BF16(0)), pick)
                rest = sums_of(jnp.where(there, low, BF16(0)).astype(F8), pick_low)
                dep[f] += sums + rest * (1.0 / LOW_SCALE)

        return body

    def deposit_loop(fields):
        wide = 8 * move
        body = deposit_stay(fields, wide)

        def step(c, carry):
            body(pl.multiple_of(c * wide, wide))
            return carry

        lax.fori_loop(0, rows // wide, step, 0)

    def arrivals(table, dim, fields):
        if dim == 0:
            along, length = table[6:7].astype(jnp.int32) - anchor_y, cells_y
        else:
            along, length = table[5:6].astype(jnp.int32) - anchor_x, cells_x
        there = picked(along, length)
        pick = jnp.where(picked(table[7:8], depth), BF16(1), BF16(0))
        parts = terms(table, fields, 1.0)
        both = jnp.concatenate(
            [jnp.where(there, s, BF16(0)) for halves in parts for s in halves], axis=0
        )
        sums = sums_of(both, pick)
        found = []
        for n in range(len(fields)):
            o = 2 * n * length
            found.append(sums[o : o + length] + sums[o + length : o + 2 * length])
        return found

    def start_all(copies, faces):
        for h in faces:
            pl.when(has[h])(copies[h].start)

    def wait_all(copies, faces):
        for h in faces:
            pl.when(has[h])(copies[h].wait_send)
            pl.when(has[h])(copies[h ^ 1].wait_recv)

    sort_parcels(
        cells_x, cells_y, anchor_x, anchor_y, mass_in, vel_in, temp_in, cell_in, count, stay, bucket
    )
    wide = rows
    for start in range(0, rows, wide):
        deposit_stay((4,), wide)(start)

    present = len(first) + len(second)
    for h in range(FACES):
        present = present + has[h].astype(jnp.int32)
    pl.semaphore_wait(barrier, present)
    sends = []
    for h in range(FACES):
        sends.append(
            pltpu.make_async_remote_copy(
                src_ref=bucket.at[h],
                dst_ref=got.at[h ^ 1],
                send_sem=bucket_send.at[h],
                recv_sem=bucket_recv.at[h ^ 1],
                device_id=near[h],
                device_id_type=MESH,
            )
        )
    start_all(sends, range(FACES))
    deposit_loop((0, 1,))
    wait_all(sends, (0, 1))
    for b, base in ((0, 0), (1, cols - cells_y)):
        for f, found in enumerate(arrivals(got[b], 0, range(5))):
            dep[f, base : base + cells_y] += found
    loads[4].wait()
    for x in range(cells_x):
        for n, y in enumerate((0, cells_y - 1)):
            here = pl.ds(x * cells_y + y, 1)
            side[n, pl.ds(x, 1)] = (ADIABATIC_INDEX - 1.0) * (ener[here] + dep[4, here])
    faces = [
        press.at[pl.ds(0, cells_y)],
        press.at[pl.ds(cols - cells_y, cells_y)],
        side.at[0],
        side.at[1],
    ]
    sides = []
    for h in range(FACES):
        sides.append(
            pltpu.make_async_remote_copy(
                src_ref=faces[h],
                dst_ref=halo.at[h ^ 1],
                send_sem=halo_send.at[h],
                recv_sem=halo_recv.at[h ^ 1],
                device_id=near[h],
                device_id_type=MESH,
            )
        )
    start_all(sides, (2, 3))
    wait_all(sends, (2, 3))
    for b in (2, 3):
        for f, found in enumerate(arrivals(got[b], 1, range(5))):
            rim[b - 2, f] = found
    y = row_iota((cells_y, depth))
    for x in range(cells_x):
        here = pl.ds(x * cells_y, cells_y)
        edge = jnp.where(y == 0, rim[0, 4, x : x + 1], 0.0)
        edge += jnp.where(y == cells_y - 1, rim[1, 4, x : x + 1], 0.0)
        total = ener[here] + (dep[4, here] + edge)
        ener[here] = total
        press[here] = (ADIABATIC_INDEX - 1.0) * total
    start_all(sides, (0, 1))
    gone = [arrivals(bucket[h], 1, (4,))[0] * (ADIABATIC_INDEX - 1.0) for h in (2, 3)]
    deposit_loop((2, 3))
    for load in loads[5:]:
        load.wait()
    wait_all(sides, range(FACES))

    low_x, high_x = halo[0], halo[1]
    low_y, high_y = halo[2] + gone[0], halo[3] + gone[1]
    z = lane_iota((cells_y, depth))
    fastest = jnp.zeros((cells_y, depth), F32)
    for x in range(cells_x):
        here = pl.ds(x * cells_y, cells_y)
        p = press[here]
        before = press[pl.ds((x - 1) * cells_y, cells_y)] if x else low_x
        after = press[pl.ds((x + 1) * cells_y, cells_y)] if x < cells_x - 1 else high_x
        below = jnp.where(y == 0, low_y[x : x + 1], pltpu.roll(p, 1, axis=0))
        above = jnp.where(y == cells_y - 1, high_y[x : x + 1], pltpu.roll(p, cells_y - 1, axis=0))
        under = jnp.where(z == 0, 0.0, pltpu.roll(p, 1, axis=1))
        over = jnp.where(z == depth - 1, 0.0, pltpu.roll(p, depth - 1, axis=1))

        def deposited(f):
            edge = jnp.where(y == 0, rim[0, f, x : x + 1], 0.0)
            edge += jnp.where(y == cells_y - 1, rim[1, f, x : x + 1], 0.0)
            return dep[f, here] + edge

        rho = dens[here] + deposited(0)
        dens[here] = rho
        speed = jnp.zeros_like(p)
        for k, (a, b) in enumerate(((before, after), (below, above), (under, over))):
            impulse = mom[k, here] + deposited(k + 1) - KICK * (0.5 * (b - a))
            mom[k, here] = impulse
            speed = jnp.maximum(speed, jnp.abs(impulse))
        wave = speed / rho + jnp.sqrt(ADIABATIC_INDEX * p / rho)
        fastest = jnp.maximum(fastest, wave)
    top = jnp.max(fastest, axis=0, keepdims=True)
    top = jnp.maximum(top[:, :128], top[:, 128:])
    for phase, peers in enumerate((first, second)):
        best[phase] = top
        copies = []
        for q, peer in enumerate(peers):
            copies.append(
                pltpu.make_async_remote_copy(
                    src_ref=best.at[phase],
                    dst_ref=best_in.at[phase, q],
                    send_sem=best_send.at[phase, q],
                    recv_sem=best_recv.at[phase, q],
                    device_id=peer,
                    device_id_type=MESH,
                )
            )
        for copy in copies:
            copy.start()
        if phase == 0:
            state_out[:, :rows] = stay[:5]
            cell_out[:, :rows] = stay[5:].astype(jnp.int32)
        else:
            for b in range(FACES):
                here = pl.ds(rows + b * move, move)
                state_out[:, here] = got[b, :5]
                cell_out[:, here] = got[b, 5:].astype(jnp.int32)
        for copy in copies:
            copy.wait()
        for q in range(len(peers)):
            top = jnp.maximum(top, best_in[phase, q])
    step_out[...] = COURANT / jnp.broadcast_to(jnp.max(top, axis=1, keepdims=True), (1, 128))


def write_kernel(*refs):
    sem = refs[-1]
    count = len(refs) // 2
    copies = [
        pltpu.make_async_copy(refs[n], refs[count + n], sem.at[n]) for n in range(count)
    ]
    for copy in copies:
        copy.start()
    for copy in copies:
        copy.wait()


def in_hbm(array):
    return pltpu.with_memory_space_constraint(array, HBM)


def on_device(density, momentum, energy, mass, velocity, temp, cell, count):
    cells_x, cells_y, depth = density.shape
    rows = mass.shape[0]
    move = rows // 16
    slots = rows + FACES * move
    cols = cells_x * cells_y
    vmem = pl.BlockSpec(memory_space=VMEM)
    far = pl.BlockSpec(memory_space=HBM)
    nx, ny = lax.axis_size("gx"), lax.axis_size("gy")
    field = jax.ShapeDtypeStruct((cols, depth), F32)
    dens, mom, ener, state, cells, step = pl.pallas_call(
        functools.partial(fused_kernel, nx, ny, cells_x, cells_y),
        name="spray_step",
        out_shape=(
            field,
            jax.ShapeDtypeStruct((3, cols, depth), F32),
            field,
            jax.ShapeDtypeStruct((5, slots), F32),
            jax.ShapeDtypeStruct((3, slots), jnp.int32),
            jax.ShapeDtypeStruct((1, 128), F32),
        ),
        in_specs=[far] * 4 + [pl.BlockSpec(memory_space=pltpu.SMEM)] + [far] * 3,
        out_specs=(vmem,) * 6,
        scratch_shapes=[
            VMEM((1, rows), F32),
            VMEM((3, rows), F32),
            VMEM((1, rows), F32),
            VMEM((3, rows), jnp.int32),
            VMEM((8, rows), F32),
            VMEM((FACES, 8, move), F32),
            VMEM((cols, depth), F32),
            VMEM((5, cols, depth), F32),
            VMEM((2, 5, cells_x, depth), F32),
            VMEM((FACES, 8, move), F32),
            VMEM((2, cells_x, depth), F32),
            VMEM((FACES, cells_y, depth), F32),
            VMEM((2, 1, 128), F32),
            VMEM((2, 15, 1, 128), F32),
            pltpu.SemaphoreType.DMA((7,)),
            pltpu.SemaphoreType.DMA((FACES,)),
            pltpu.SemaphoreType.DMA((FACES,)),
            pltpu.SemaphoreType.DMA((FACES,)),
            pltpu.SemaphoreType.DMA((FACES,)),
            pltpu.SemaphoreType.DMA((2, 15)),
            pltpu.SemaphoreType.DMA((2, 15)),
        ],
        compiler_params=pltpu.CompilerParams(
            vmem_limit_bytes=32 * 2**20, collective_id=0, has_side_effects=True
        ),
    )(
        in_hbm(mass.reshape(1, rows)),
        in_hbm(velocity),
        in_hbm(temp.reshape(1, rows)),
        in_hbm(cell),
        count,
        in_hbm(density.reshape(cols, depth)),
        in_hbm(momentum.reshape(3, cols, depth)),
        in_hbm(energy.reshape(cols, depth)),
    )
    results = (dens, mom, ener, state, cells, step)
    dens, mom, ener, state, cells, step = pl.pallas_call(
        write_kernel,
        name="write_results",
        out_shape=tuple(jax.ShapeDtypeStruct(r.shape, r.dtype) for r in results),
        in_specs=[vmem] * 6,
        out_specs=(far,) * 6,
        scratch_shapes=[pltpu.SemaphoreType.DMA((6,))],
        compiler_params=pltpu.CompilerParams(vmem_limit_bytes=2**20),
    )(*results)
    return (
        dens.reshape(density.shape),
        mom.reshape(momentum.shape),
        ener.reshape(energy.shape),
        state,
        cells,
        step[0, 0],
    )


def solution(mesh):
    both = ("gx", "gy")
    return jax.shard_map(
        on_device,
        mesh=mesh,
        in_specs=(
            P("gx", "gy", None),
            P(None, "gx", "gy", None),
            P("gx", "gy", None),
            P(both),
            P(None, both),
            P(both),
            P(None, both),
            P(both),
        ),
        out_specs=(
            P("gx", "gy", None),
            P(None, "gx", "gy", None),
            P("gx", "gy", None),
            P(None, both),
            P(None, both),
            P(),
        ),
        check_vma=False,
    )
```

```python
import functools

import jax
import jax.numpy as jnp
from jax import lax
from jax.experimental import pallas as pl
from jax.experimental.pallas import tpu as pltpu
from jax.sharding import PartitionSpec as P

ADIABATIC_INDEX = 1.4
KICK = 0.25
COURANT = 0.4
SHRINK = 0.5
FACES = 4
F32 = jnp.float32
BF16 = jnp.bfloat16
F8 = jnp.float8_e4m3fn
LOW_SCALE = 2048.0
MESH = pl.DeviceIdType.MESH
VMEM = pltpu.VMEM
HBM = pltpu.HBM


def row_iota(shape):
    return lax.broadcasted_iota(jnp.int32, shape, 0)


def lane_iota(shape):
    return lax.broadcasted_iota(jnp.int32, shape, 1)


def folded(row, parts):
    width = row.shape[1] // parts
    pieces = [
        row[r : r + 1, k * width : (k + 1) * width]
        for r in range(row.shape[0])
        for k in range(parts)
    ]
    return jnp.concatenate(pieces, axis=0)


def folded_left(fold, step):
    width = fold.shape[1]
    if step >= width:
        return pltpu.roll(fold, 8 - step // width, axis=0)
    near = pltpu.roll(fold, width - step, axis=1)
    return jnp.where(lane_iota(fold.shape) >= width - step, pltpu.roll(near, 7, axis=0), near)


def pack_left(cells, shift, steps):
    width = cells.shape[1]
    part = shift.shape[1]
    for k in range(steps):
        step = 1 << k
        coming_shift = folded_left(shift, step)
        take = coming_shift & step
        shift = jnp.where(take != 0, coming_shift, jnp.where((shift & step) != 0, 0, shift))
        spread = jnp.concatenate(
            [jnp.broadcast_to(take[r : r + 1], (8, part)) for r in range(8)], axis=1
        )
        cells = jnp.where(spread != 0, pltpu.roll(cells, width - step, axis=1), cells)
    return cells, shift


def sort_parcels(
    cells_x, cells_y, anchor_x, anchor_y, mass, vel, temp, cell, count, stay_out, bucket_out
):
    rows = mass.shape[1]
    move = rows // 16
    chunk = 256
    chunks = rows // chunk
    live = lane_iota((1, rows)) < count[0]
    m, t = mass[...], temp[...]
    boiled = m * (1.0 / (1.0 + jnp.exp(4.0 - 2.0 * t)))
    left = m - SHRINK * boiled
    local_x = cell[0:1, :] - anchor_x
    local_y = cell[1:2, :] - anchor_y
    heading = jnp.where(
        local_x < 0,
        0,
        jnp.where(
            local_x >= cells_x, 1, jnp.where(local_y < 0, 2, jnp.where(local_y >= cells_y, 3, 4))
        ),
    )
    heading = jnp.where(live, heading, 5)
    record = jnp.concatenate([left, vel[...], t, cell[...].astype(F32)], axis=0)
    heads = jnp.broadcast_to(heading, (8, rows))
    stay_out[...] = jnp.where(heads == 4, record, 0.0)

    sub = row_iota((8, rows))
    mask = jnp.where((sub == heads) & (sub < 4), 1.0, 0.0)
    mask = jnp.where((sub == 4) & (heads < 4), 1.0, mask)
    stacked = jnp.concatenate(
        [mask[:, c * chunk : (c + 1) * chunk] for c in range(chunks)], axis=0
    ).astype(BF16)
    a, b = row_iota((chunk, chunk)), lane_iota((chunk, chunk))
    upper = jnp.where(a < b, 1.0, 0.0).astype(BF16)
    inside = jnp.dot(stacked, upper, preferred_element_type=F32)
    total = jnp.dot(stacked, jnp.ones((chunk, chunk), BF16), preferred_element_type=F32)
    n = 8 * chunks
    a, b = row_iota((n, n)), lane_iota((n, n))
    ahead = jnp.where(((a & 7) == (b & 7)) & (b < a), 1.0, 0.0).astype(BF16)
    before = jnp.dot(ahead, total.astype(BF16), preferred_element_type=F32)
    ranks = inside + before
    rank = jnp.concatenate([ranks[c * 8 : (c + 1) * 8] for c in range(chunks)], axis=1)
    counts = (before + total)[n - 8 : n, :128].astype(jnp.int32)

    own = jnp.sum(jnp.where(sub < 4, mask * rank, 0.0), axis=0, keepdims=True).astype(jnp.int32)
    overall = rank[4:5].astype(jnp.int32)
    moves = heading < 4
    shift = lane_iota((1, rows)) - overall
    target = heading * move + own
    shift = jnp.where(moves, shift + target * rows, 0)
    packed, key = pack_left(record, folded(shift, 8), rows.bit_length() - 1)

    wide = FACES * move
    eighth = wide // 8
    packed = packed[:, :wide]
    lead = wide * 8 // rows
    slot = folded(key[:lead], 8 // lead) // rows
    place = row_iota((8, eighth)) * eighth + lane_iota((8, eighth))
    movers = jnp.concatenate([counts[4:5]] * (eighth // 128), axis=1)
    present = place < jnp.broadcast_to(movers, (8, eighth))
    for h in range(FACES):
        mine = present & (slot // move == h)
        gap = jnp.where(mine, place - (slot - h * move), 0)
        out, _ = pack_left(packed, gap, wide.bit_length() - 1)
        full = jnp.concatenate([counts[h : h + 1]] * (move // 128), axis=1)
        bucket_out[h] = jnp.where(lane_iota((8, move)) < full, out[:, :move], 0.0)


def fused_kernel(
    nx,
    ny,
    cells_x,
    cells_y,
    mass,
    vel,
    temp,
    cell,
    count,
    density,
    momentum,
    energy,
    dens,
    mom,
    ener,
    state_out,
    cell_out,
    step_out,
    mass_in,
    vel_in,
    temp_in,
    cell_in,
    stay,
    bucket,
    press,
    dep,
    rim,
    got,
    side,
    halo,
    best,
    best_in,
    load_sem,
    bucket_send,
    bucket_recv,
    halo_send,
    halo_recv,
    best_send,
    best_recv,
):
    i, j = lax.axis_index("gx"), lax.axis_index("gy")
    cols = cells_x * cells_y
    depth = press.shape[1]
    rows = stay.shape[1]
    move = got.shape[2]
    up_x, down_x = lax.rem(i + 1, nx), lax.rem(i + nx - 1, nx)
    up_y, down_y = lax.rem(j + 1, ny), lax.rem(j + ny - 1, ny)
    near = [(down_x, j), (up_x, j), (i, down_y), (i, up_y)]
    has = [i > 0, i < nx - 1, j > 0, j < ny - 1]
    half = ny // 2
    spot = lax.div(j, half) * nx + i
    lane = lax.rem(j, half)
    size_a, size_b = 2 * nx, half
    first = []
    for q in range(1, size_a):
        there = lax.rem(spot + q, size_a)
        first.append((lax.rem(there, nx), lax.div(there, nx) * half + lane))
    second = []
    for q in range(1, size_b):
        second.append((i, lax.div(j, half) * half + lax.rem(lane + q, size_b)))

    pairs = [
        (cell, cell_in),
        (mass, mass_in),
        (temp, temp_in),
        (vel, vel_in),
        (energy, ener),
        (density, dens),
        (momentum, mom),
    ]
    loads = [
        pltpu.make_async_copy(src, dst, load_sem.at[n]) for n, (src, dst) in enumerate(pairs)
    ]
    for load in loads:
        load.start()

    barrier = pltpu.get_barrier_semaphore()
    for peer in first + second:
        pl.semaphore_signal(barrier, inc=1, device_id=peer, device_id_type=MESH)
    for h in range(FACES):

        @pl.when(has[h])
        def _():
            pl.semaphore_signal(barrier, inc=1, device_id=near[h], device_id_type=MESH)

        @pl.when(jnp.logical_not(has[h]))
        def _():
            got[h] = jnp.zeros_like(got[h])
            halo[h] = jnp.zeros_like(halo[h])

    dep[...] = jnp.zeros_like(dep)
    for load in loads[:4]:
        load.wait()

    anchor_x, anchor_y = i * cells_x, j * cells_y
    def terms(table, fields, scale):
        v = table[1:4]
        t = table[4:5]
        boiled = table[0:1] / (0.5 + jnp.exp(4.0 - 2.0 * t))
        parts = []
        for f in fields:
            if f == 0:
                s = boiled
            elif f < 4:
                s = boiled * v[f - 1 : f]
            else:
                s = boiled * (t + 0.5 * jnp.sum(v * v, axis=0, keepdims=True))
            high = s.astype(BF16)
            low = ((s - high.astype(F32)) * scale).astype(BF16)
            parts.append((high, low))
        return parts

    def picked(index, size):
        which = row_iota((size, index.shape[1])).astype(F32).astype(BF16)
        return which == index.astype(F32).astype(BF16)

    def sums_of(both, pick):
        return lax.dot_general(both, pick, (((1,), (1,)), ((), ())), preferred_element_type=F32)

    def deposit_stay(fields, wide):
        def body(start):
            table = stay[:, pl.ds(start, wide)]
            parts = terms(table, fields, LOW_SCALE)
            local_x = table[5:6].astype(jnp.int32) - anchor_x
            local_y = table[6:7].astype(jnp.int32) - anchor_y
            there = picked(local_x * cells_y + local_y, cols)
            pick = jnp.where(picked(table[7:8], depth), BF16(1), BF16(0))
            pick_low = pick.astype(F8)
            for f, (high, low) in zip(fields, parts):
                sums = sums_of(jnp.where(there, high, BF16(0)), pick)
                rest = sums_of(jnp.where(there, low, BF16(0)).astype(F8), pick_low)
                dep[f] += sums + rest * (1.0 / LOW_SCALE)

        return body

    def deposit_loop(fields):
        wide = 8 * move
        body = deposit_stay(fields, wide)

        def step(c, carry):
            body(pl.multiple_of(c * wide, wide))
            return carry

        lax.fori_loop(0, rows // wide, step, 0)

    def arrivals(table, dim, fields):
        if dim == 0:
            along, length = table[6:7].astype(jnp.int32) - anchor_y, cells_y
        else:
            along, length = table[5:6].astype(jnp.int32) - anchor_x, cells_x
        there = picked(along, length)
        pick = jnp.where(picked(table[7:8], depth), BF16(1), BF16(0))
        parts = terms(table, fields, 1.0)
        both = jnp.concatenate(
            [jnp.where(there, s, BF16(0)) for halves in parts for s in halves], axis=0
        )
        sums = sums_of(both, pick)
        found = []
        for n in range(len(fields)):
            o = 2 * n * length
            found.append(sums[o : o + length] + sums[o + length : o + 2 * length])
        return found

    def start_all(copies, faces):
        for h in faces:
            pl.when(has[h])(copies[h].start)

    def wait_all(copies, faces):
        for h in faces:
            pl.when(has[h])(copies[h].wait_send)
            pl.when(has[h])(copies[h ^ 1].wait_recv)

    sort_parcels(
        cells_x, cells_y, anchor_x, anchor_y, mass_in, vel_in, temp_in, cell_in, count, stay, bucket
    )
    wide = rows
    for start in range(0, rows, wide):
        deposit_stay((4,), wide)(start)

    present = len(first) + len(second)
    for h in range(FACES):
        present = present + has[h].astype(jnp.int32)
    pl.semaphore_wait(barrier, present)
    sends = []
    for h in range(FACES):
        sends.append(
            pltpu.make_async_remote_copy(
                src_ref=bucket.at[h],
                dst_ref=got.at[h ^ 1],
                send_sem=bucket_send.at[h],
                recv_sem=bucket_recv.at[h ^ 1],
                device_id=near[h],
                device_id_type=MESH,
            )
        )
    start_all(sends, (2, 3, 0, 1))
    deposit_loop((0, 1,))
    wait_all(sends, (0, 1))
    for b, base in ((0, 0), (1, cols - cells_y)):
        for f, found in enumerate(arrivals(got[b], 0, range(5))):
            dep[f, base : base + cells_y] += found
    loads[4].wait()
    for x in range(cells_x):
        for n, y in enumerate((0, cells_y - 1)):
            here = pl.ds(x * cells_y + y, 1)
            side[n, pl.ds(x, 1)] = (ADIABATIC_INDEX - 1.0) * (ener[here] + dep[4, here])
    faces = [
        press.at[pl.ds(0, cells_y)],
        press.at[pl.ds(cols - cells_y, cells_y)],
        side.at[0],
        side.at[1],
    ]
    sides = []
    for h in range(FACES):
        sides.append(
            pltpu.make_async_remote_copy(
                src_ref=faces[h],
                dst_ref=halo.at[h ^ 1],
                send_sem=halo_send.at[h],
                recv_sem=halo_recv.at[h ^ 1],
                device_id=near[h],
                device_id_type=MESH,
            )
        )
    start_all(sides, (2, 3))
    y = row_iota((cells_y, depth))
    long_way = (j == half - 1) | (j == half)

    def finish_energy():
        wait_all(sends, (2, 3))
        for b in (2, 3):
            for f, found in enumerate(arrivals(got[b], 1, range(5))):
                rim[b - 2, f] = found
        for x in range(cells_x):
            here = pl.ds(x * cells_y, cells_y)
            edge = jnp.where(y == 0, rim[0, 4, x : x + 1], 0.0)
            edge += jnp.where(y == cells_y - 1, rim[1, 4, x : x + 1], 0.0)
            total = ener[here] + (dep[4, here] + edge)
            ener[here] = total
            press[here] = (ADIABATIC_INDEX - 1.0) * total
        start_all(sides, (0, 1))

    pl.when(jnp.logical_not(long_way))(finish_energy)
    gone = [arrivals(bucket[h], 1, (4,))[0] * (ADIABATIC_INDEX - 1.0) for h in (2, 3)]
    deposit_loop((2, 3))
    pl.when(long_way)(finish_energy)
    for load in loads[5:]:
        load.wait()
    wait_all(sides, range(FACES))

    low_x, high_x = halo[0], halo[1]
    low_y, high_y = halo[2] + gone[0], halo[3] + gone[1]
    z = lane_iota((cells_y, depth))
    fastest = jnp.zeros((cells_y, depth), F32)
    for x in range(cells_x):
        here = pl.ds(x * cells_y, cells_y)
        p = press[here]
        before = press[pl.ds((x - 1) * cells_y, cells_y)] if x else low_x
        after = press[pl.ds((x + 1) * cells_y, cells_y)] if x < cells_x - 1 else high_x
        below = jnp.where(y == 0, low_y[x : x + 1], pltpu.roll(p, 1, axis=0))
        above = jnp.where(y == cells_y - 1, high_y[x : x + 1], pltpu.roll(p, cells_y - 1, axis=0))
        under = jnp.where(z == 0, 0.0, pltpu.roll(p, 1, axis=1))
        over = jnp.where(z == depth - 1, 0.0, pltpu.roll(p, depth - 1, axis=1))

        def deposited(f):
            edge = jnp.where(y == 0, rim[0, f, x : x + 1], 0.0)
            edge += jnp.where(y == cells_y - 1, rim[1, f, x : x + 1], 0.0)
            return dep[f, here] + edge

        rho = dens[here] + deposited(0)
        dens[here] = rho
        speed = jnp.zeros_like(p)
        for k, (a, b) in enumerate(((before, after), (below, above), (under, over))):
            impulse = mom[k, here] + deposited(k + 1) - KICK * (0.5 * (b - a))
            mom[k, here] = impulse
            speed = jnp.maximum(speed, jnp.abs(impulse))
        wave = speed / rho + jnp.sqrt(ADIABATIC_INDEX * p / rho)
        fastest = jnp.maximum(fastest, wave)
    top = jnp.max(fastest, axis=0, keepdims=True)
    top = jnp.maximum(top[:, :128], top[:, 128:])
    for phase, peers in enumerate((first, second)):
        best[phase] = top
        copies = []
        for q, peer in enumerate(peers):
            copies.append(
                pltpu.make_async_remote_copy(
                    src_ref=best.at[phase],
                    dst_ref=best_in.at[phase, q],
                    send_sem=best_send.at[phase, q],
                    recv_sem=best_recv.at[phase, q],
                    device_id=peer,
                    device_id_type=MESH,
                )
            )
        for copy in copies:
            copy.start()
        if phase == 0:
            state_out[:, :rows] = stay[:5]
            cell_out[:, :rows] = stay[5:].astype(jnp.int32)
        else:
            for b in range(FACES):
                here = pl.ds(rows + b * move, move)
                state_out[:, here] = got[b, :5]
                cell_out[:, here] = got[b, 5:].astype(jnp.int32)
        for copy in copies:
            copy.wait()
        for q in range(len(peers)):
            top = jnp.maximum(top, best_in[phase, q])
    step_out[...] = COURANT / jnp.broadcast_to(jnp.max(top, axis=1, keepdims=True), (1, 128))


def write_kernel(*refs):
    sem = refs[-1]
    count = len(refs) // 2
    copies = [
        pltpu.make_async_copy(refs[n], refs[count + n], sem.at[n]) for n in range(count)
    ]
    for copy in copies:
        copy.start()
    for copy in copies:
        copy.wait()


def in_hbm(array):
    return pltpu.with_memory_space_constraint(array, HBM)


def on_device(density, momentum, energy, mass, velocity, temp, cell, count):
    cells_x, cells_y, depth = density.shape
    rows = mass.shape[0]
    move = rows // 16
    slots = rows + FACES * move
    cols = cells_x * cells_y
    vmem = pl.BlockSpec(memory_space=VMEM)
    far = pl.BlockSpec(memory_space=HBM)
    nx, ny = lax.axis_size("gx"), lax.axis_size("gy")
    field = jax.ShapeDtypeStruct((cols, depth), F32)
    dens, mom, ener, state, cells, step = pl.pallas_call(
        functools.partial(fused_kernel, nx, ny, cells_x, cells_y),
        name="spray_step",
        out_shape=(
            field,
            jax.ShapeDtypeStruct((3, cols, depth), F32),
            field,
            jax.ShapeDtypeStruct((5, slots), F32),
            jax.ShapeDtypeStruct((3, slots), jnp.int32),
            jax.ShapeDtypeStruct((1, 128), F32),
        ),
        in_specs=[far] * 4 + [pl.BlockSpec(memory_space=pltpu.SMEM)] + [far] * 3,
        out_specs=(vmem,) * 6,
        scratch_shapes=[
            VMEM((1, rows), F32),
            VMEM((3, rows), F32),
            VMEM((1, rows), F32),
            VMEM((3, rows), jnp.int32),
            VMEM((8, rows), F32),
            VMEM((FACES, 8, move), F32),
            VMEM((cols, depth), F32),
            VMEM((5, cols, depth), F32),
            VMEM((2, 5, cells_x, depth), F32),
            VMEM((FACES, 8, move), F32),
            VMEM((2, cells_x, depth), F32),
            VMEM((FACES, cells_y, depth), F32),
            VMEM((2, 1, 128), F32),
            VMEM((2, 15, 1, 128), F32),
            pltpu.SemaphoreType.DMA((7,)),
            pltpu.SemaphoreType.DMA((FACES,)),
            pltpu.SemaphoreType.DMA((FACES,)),
            pltpu.SemaphoreType.DMA((FACES,)),
            pltpu.SemaphoreType.DMA((FACES,)),
            pltpu.SemaphoreType.DMA((2, 15)),
            pltpu.SemaphoreType.DMA((2, 15)),
        ],
        compiler_params=pltpu.CompilerParams(
            vmem_limit_bytes=32 * 2**20, collective_id=0, has_side_effects=True
        ),
    )(
        in_hbm(mass.reshape(1, rows)),
        in_hbm(velocity),
        in_hbm(temp.reshape(1, rows)),
        in_hbm(cell),
        count,
        in_hbm(density.reshape(cols, depth)),
        in_hbm(momentum.reshape(3, cols, depth)),
        in_hbm(energy.reshape(cols, depth)),
    )
    results = (dens, mom, ener, state, cells, step)
    dens, mom, ener, state, cells, step = pl.pallas_call(
        write_kernel,
        name="write_results",
        out_shape=tuple(jax.ShapeDtypeStruct(r.shape, r.dtype) for r in results),
        in_specs=[vmem] * 6,
        out_specs=(far,) * 6,
        scratch_shapes=[pltpu.SemaphoreType.DMA((6,))],
        compiler_params=pltpu.CompilerParams(vmem_limit_bytes=2**20),
    )(*results)
    return (
        dens.reshape(density.shape),
        mom.reshape(momentum.shape),
        ener.reshape(energy.shape),
        state,
        cells,
        step[0, 0],
    )


def solution(mesh):
    both = ("gx", "gy")
    return jax.shard_map(
        on_device,
        mesh=mesh,
        in_specs=(
            P("gx", "gy", None),
            P(None, "gx", "gy", None),
            P("gx", "gy", None),
            P(both),
            P(None, both),
            P(both),
            P(None, both),
            P(both),
        ),
        out_specs=(
            P("gx", "gy", None),
            P(None, "gx", "gy", None),
            P("gx", "gy", None),
            P(None, both),
            P(None, both),
            P(),
        ),
        check_vma=False,
    )
```
